256 devices in a mesh: crop: 4 (over z_hi, core), row: 64 (over y, x, z_lo).
Axes of the slice: x: 4, y: 4, z: 8 (z_hi: 2, z_lo: 4; z = z_hi * 4 + z_lo), core: 2. Of those that a mesh axis runs over, the one named last changes fastest.
Arguments:
- pair: bfloat16 [4, 512, 512, 128], P('crop', 'row'), may hold values from -6 to 6
- cotangent: bfloat16 [4, 512, 512, 128], P('crop', 'row'), may hold values from -6 to 6
- lengths: int32 [4], P('crop'), may hold values from 256 to 512
- proj_weight: bfloat16 [128, 640], replicated, may hold values from -0.5 to 0.5
- out_weight: bfloat16 [128, 128], replicated, may hold values from -0.5 to 0.5
- up_weight: bfloat16 [128, 512], replicated, may hold values from -0.5 to 0.5
- down_weight: bfloat16 [512, 128], replicated, may hold values from -0.25 to 0.25
- norm_gain: float32 [3, 128], replicated, may hold values from 0.1 to 1.9
- norm_bias: float32 [3, 128], replicated, may hold values from -3 to 3
Outputs:
- grad_pair: bfloat16 [4, 512, 512, 128], P('crop', 'row')
- grad_proj: float32 [128, 640], replicated
- grad_out: float32 [128, 128], replicated
- grad_up: float32 [128, 512], replicated
- grad_down: float32 [512, 128], replicated
- grad_gain: float32 [3, 128], replicated
- grad_bias: float32 [3, 128], replicated
The draws below stay inside these ranges and needn't reach their ends.
Inputs may be any that keep to these rules, and one draw needn't show every extreme that they name: lengths[s] residues of crop s are present; the rest are masked.
All inputs are finite; a program needn't handle non-finite values.
Results may differ from the reference program's by a relative error of at most 0.009.
Values may be sent and summed in bfloat16 or wider, within the bound.
A program may use at most 128 MiB of HBM per device.

```python
import jax
import jax.numpy as jnp
from jax import lax

CH = 128
HID = 512
L = 512
CROPS = 4


def set_ends(drawn, stream_key, smallest, largest):
    longest = drawn.shape.index(max(drawn.shape))
    spots = []
    for shift in (0, 1):
        where = [jax.random.randint(jax.random.fold_in(stream_key, axis), (), 0, length) for axis, length in enumerate(drawn.shape)]
        where[longest] = (where[longest] + shift) % drawn.shape[longest]
        spots.append(tuple(where))
    return drawn.at[spots[0]].set(smallest).at[spots[1]].set(largest)


def block_scale(stream_key, extent, pieces, low, top_value):
    loudness = 1.0
    for dim, shards_of in pieces:
        steps = jax.random.uniform(jax.random.fold_in(jax.random.fold_in(stream_key, 6), dim), (shards_of,), jnp.float32, low / len(pieces), top_value / len(pieces))
        loudness = loudness * jnp.repeat(jnp.exp(steps), extent[dim] // shards_of).reshape((-1,) + (1,) * (len(extent) - 1 - dim))
    return loudness


def gaussian(rng, shape, width, most, pieces=(), kind=jnp.bfloat16):
    level = block_scale(rng, shape, pieces, -0.22, 0.18) if pieces else 1.0
    values = jax.random.normal(rng, shape, jnp.float32) * width * level
    return jnp.minimum(jnp.maximum(values, -most), most).astype(kind)


def setup_inputs(seed: int = 0) -> dict:
    streams_of = jax.random.split(jax.random.key(seed), 10)
    pair = gaussian(streams_of[0], (CROPS, L, L, CH), 1.0, 6.0, ((0, 4), (1, 64)))
    cotangent = gaussian(streams_of[1], (CROPS, L, L, CH), 1.0, 6.0, ((0, 4), (1, 64)))
    lengths = set_ends(jax.random.randint(streams_of[2], (CROPS,), L // 2, L + 1), jax.random.fold_in(streams_of[2], 1), L // 2, L).astype(jnp.int32)
    proj_weight = gaussian(streams_of[3], (CH, 5 * CH), CH ** -0.5, 0.5)
    out_weight = gaussian(streams_of[4], (CH, CH), CH ** -0.5, 0.5)
    up_weight = gaussian(streams_of[5], (CH, HID), CH ** -0.5, 0.5)
    down_weight = gaussian(streams_of[6], (HID, CH), HID ** -0.5, 0.25)
    norm_gain = jnp.clip(1.0 + 0.18 * jax.random.normal(streams_of[7], (3, CH), jnp.float32), 0.1, 1.9)
    norm_bias = gaussian(streams_of[8], (3, CH), 0.5, 3.0, (), jnp.float32)
    return dict(pair=pair, cotangent=cotangent, lengths=lengths, proj_weight=proj_weight, out_weight=out_weight, up_weight=up_weight, down_weight=down_weight, norm_gain=norm_gain, norm_bias=norm_bias)


EPSILON = 1e-05

def contract(pattern, left_side, right_side):
    return jnp.einsum(pattern, left_side.astype(jnp.float32), right_side.astype(jnp.float32))

def norm_forward(values, gain_vec, bias_vec, norm_axis):
    center = values - lax.optimization_barrier(jnp.mean(values, axis=norm_axis, keepdims=True))
    inv_std = lax.rsqrt(lax.optimization_barrier(jnp.mean(center * center, axis=norm_axis, keepdims=True)) + EPSILON)
    normed = center * inv_std
    return (normed, inv_std, normed * gain_vec + bias_vec)

def norm_backward(upstream, normed, inv_std, gain_vec, norm_axis, others):
    grad_gain = lax.optimization_barrier(jnp.sum(upstream * normed, axis=others))
    grad_bias = lax.optimization_barrier(jnp.sum(upstream, axis=others))
    scaled = upstream * gain_vec
    result = inv_std * (scaled - lax.optimization_barrier(jnp.mean(scaled, axis=norm_axis, keepdims=True)) - normed * lax.optimization_barrier(jnp.mean(scaled * normed, axis=norm_axis, keepdims=True)))
    return (result, grad_gain, grad_bias)

def enter_rows(pair_rows, row_keep, col_keep, proj_weight, norm_gain, norm_bias):
    channels = pair_rows.shape[2]
    normed_in, inv_in, scaled_in = norm_forward(pair_rows.astype(jnp.float32), norm_gain[0], norm_bias[0], 2)
    input_bf = scaled_in.astype(jnp.bfloat16)
    factor_pre = contract('rld,de->erl', input_bf, proj_weight[:, :4 * channels])
    gate_pre = contract('rld,de->rle', input_bf, proj_weight[:, 4 * channels:])
    keep_both = row_keep[:, None] * col_keep[None, :]
    left_bf = (jax.nn.sigmoid(factor_pre[:channels]) * factor_pre[channels:2 * channels] * keep_both).astype(jnp.bfloat16)
    right_bf = (jax.nn.sigmoid(factor_pre[2 * channels:3 * channels]) * factor_pre[3 * channels:] * keep_both).astype(jnp.bfloat16)
    return (input_bf, normed_in, inv_in, factor_pre, gate_pre, keep_both, left_bf, right_bf)

def middle_rows(pair_rows, cot_rows, product_bf, gate_pre, out_weight, up_weight, down_weight, norm_gain, norm_bias):
    prod_normed, prod_inv, prod_scaled = norm_forward(product_bf.astype(jnp.float32), norm_gain[1][:, None, None], norm_bias[1][:, None, None], 0)
    prod_norm_bf = prod_scaled.astype(jnp.bfloat16)
    update = contract('crj,cd->rjd', prod_norm_bf, out_weight)
    gate_sig = jax.nn.sigmoid(gate_pre)
    first_bf = (pair_rows.astype(jnp.float32) + gate_sig * update).astype(jnp.bfloat16)
    tran_normed, tran_inv, tran_scaled = norm_forward(first_bf.astype(jnp.float32), norm_gain[2], norm_bias[2], 2)
    tran_bf = tran_scaled.astype(jnp.bfloat16)
    hidden_pre = contract('rld,dh->rlh', tran_bf, up_weight)
    hidden_sig = jax.nn.sigmoid(hidden_pre)
    hidden_bf = (hidden_pre * hidden_sig).astype(jnp.bfloat16)
    grad_down = contract('rlh,rld->hd', hidden_bf, cot_rows)
    hidden_grad_bf = (contract('rld,hd->rlh', cot_rows, down_weight) * hidden_sig * (1.0 + hidden_pre * (1.0 - hidden_sig))).astype(jnp.bfloat16)
    grad_up = contract('rld,rlh->dh', tran_bf, hidden_grad_bf)
    tran_grad = contract('rlh,dh->rld', hidden_grad_bf, up_weight)
    first_grad, gain_tran, bias_tran = norm_backward(tran_grad, tran_normed, tran_inv, norm_gain[2], 2, (0, 1))
    first_grad = first_grad + cot_rows.astype(jnp.float32)
    update_grad_bf = (first_grad * gate_sig).astype(jnp.bfloat16)
    gate_grad_bf = (first_grad * update * gate_sig * (1.0 - gate_sig)).astype(jnp.bfloat16)
    grad_out = contract('crj,rjd->cd', prod_norm_bf, update_grad_bf)
    norm_grad = contract('rjd,cd->crj', update_grad_bf, out_weight)
    prod_grad, gain_prod, bias_prod = norm_backward(norm_grad, prod_normed, prod_inv, norm_gain[1][:, None, None], 0, (1, 2))
    return (prod_grad.astype(jnp.bfloat16), first_grad, gate_grad_bf, grad_out, grad_up, grad_down, gain_prod, bias_prod, gain_tran, bias_tran)

def leave_rows(left_grad, right_grad, factor_pre, keep_both, gate_grad_bf, input_bf, normed_in, inv_in, first_grad, proj_weight, norm_gain):
    channels = gate_grad_bf.shape[2]
    sig_left = jax.nn.sigmoid(factor_pre[:channels])
    lin_left = factor_pre[channels:2 * channels]
    sig_right = jax.nn.sigmoid(factor_pre[2 * channels:3 * channels])
    lin_right = factor_pre[3 * channels:]
    masked_left = left_grad.astype(jnp.float32) * keep_both
    masked_right = right_grad.astype(jnp.float32) * keep_both
    factor_grad = jnp.concatenate([masked_left * lin_left * sig_left * (1.0 - sig_left), masked_left * sig_left, masked_right * lin_right * sig_right * (1.0 - sig_right), masked_right * sig_right], axis=0).astype(jnp.bfloat16)
    grad_proj = jnp.concatenate([contract('rld,erl->de', input_bf, factor_grad), contract('rld,rle->de', input_bf, gate_grad_bf)], axis=1)
    input_grad = contract('erl,de->rld', factor_grad, proj_weight[:, :4 * channels]) + contract('rle,de->rld', gate_grad_bf, proj_weight[:, 4 * channels:])
    pair_grad, gain_in, bias_in = norm_backward(input_grad, normed_in, inv_in, norm_gain[0], 2, (0, 1))
    return ((pair_grad + first_grad).astype(jnp.bfloat16), grad_proj, gain_in, bias_in)

def reference(pair, cotangent, lengths, proj_weight, out_weight, up_weight, down_weight, norm_gain, norm_bias):

    def one_crop(operands):
        pair_crop, cot_crop, length = operands
        row_keep = (jnp.arange(L, dtype=jnp.int32) < length).astype(jnp.float32)
        entered = enter_rows(pair_crop, row_keep, row_keep, proj_weight, norm_gain, norm_bias)
        input_bf, normed_in, inv_in, factor_pre, gate_pre, keep_both, left_bf, right_bf = entered
        product_bf = contract('cik,cjk->cij', left_bf, right_bf).astype(jnp.bfloat16)
        middle = middle_rows(pair_crop, cot_crop, product_bf, gate_pre, out_weight, up_weight, down_weight, norm_gain, norm_bias)
        prod_grad_bf, first_grad, gate_grad_bf, grad_out, grad_up, grad_down, gain_prod, bias_prod, gain_tran, bias_tran = middle
        left_grad = contract('cij,cjk->cik', prod_grad_bf, right_bf).astype(jnp.bfloat16)
        right_grad = contract('cij,cik->cjk', prod_grad_bf, left_bf).astype(jnp.bfloat16)
        pair_grad, grad_proj, gain_in, bias_in = leave_rows(left_grad, right_grad, factor_pre, keep_both, gate_grad_bf, input_bf, normed_in, inv_in, first_grad, proj_weight, norm_gain)
        return (pair_grad, grad_proj, grad_out, grad_up, grad_down, jnp.stack([gain_in, gain_prod, gain_tran]), jnp.stack([bias_in, bias_prod, bias_tran]))
    results = lax.map(one_crop, (pair, cotangent, lengths))
    factor = 1.0 / L
    return (results[0], lax.optimization_barrier(jnp.sum(results[1], axis=0)) * factor, lax.optimization_barrier(jnp.sum(results[2], axis=0)) * factor, lax.optimization_barrier(jnp.sum(results[3], axis=0)) * factor, lax.optimization_barrier(jnp.sum(results[4], axis=0)) * factor, lax.optimization_barrier(jnp.sum(results[5], axis=0)) * factor, lax.optimization_barrier(jnp.sum(results[6], axis=0)) * factor)
```

```python
import functools

import jax
import jax.numpy as jnp
from jax import lax
from jax.experimental import pallas as pl
from jax.experimental.pallas import tpu as pltpu
from jax.sharding import PartitionSpec as P

F32 = jnp.float32
MESH = pl.DeviceIdType.MESH

EPSILON = 1e-05


def side_by_side(arrays, axis, split_dim, concat_dim, along):
    widths = [a.shape[along] for a in arrays]
    both = jnp.concatenate(arrays, axis=along)
    filled = lax.all_to_all(both, axis, split_axis=split_dim, concat_axis=concat_dim, tiled=True)
    return tuple(jnp.split(filled, [sum(widths[:k]) for k in range(1, len(widths))], axis=along))


def place():
    crop = lax.axis_index("crop")
    row = lax.axis_index("row")
    core = lax.rem(crop, 2)
    zhi = lax.div(crop, 2)
    q = lax.div(row, 4)
    zlo = lax.rem(row, 4)
    return core, zhi * 4 + zlo, q


def device_at(core, z, q):
    return (lax.div(z, 4) * 2 + core, q * 4 + lax.rem(z, 4))


def send(src, dst, send_sem, recv_sem, device):
    return pltpu.make_async_remote_copy(
        src_ref=src,
        dst_ref=dst,
        send_sem=send_sem,
        recv_sem=recv_sem,
        device_id=device,
        device_id_type=MESH,
    )


def wait_for(ref, sem):
    pltpu.make_async_copy(ref, ref, sem).wait()


def reduce_kernel(scale, x_ref, o_ref, from_core, from_plane, from_z, half, part, piece, all_z, all_plane, all_core, send_sems, recv_sems):
    core, z, q = place()
    partner = device_at(1 - core, z, q)
    barrier = pltpu.get_barrier_semaphore()
    pl.semaphore_signal(barrier, inc=1, device_id=partner, device_id_type=MESH)

    def greet_plane(p, carry):
        pl.semaphore_signal(barrier, inc=1, device_id=device_at(core, z, lax.rem(q + p, 16)), device_id_type=MESH)
        return carry

    def greet_z(p, carry):
        pl.semaphore_signal(barrier, inc=1, device_id=device_at(core, lax.rem(z + p, 8), q), device_id_type=MESH)
        return carry

    lax.fori_loop(1, 16, greet_plane, 0)
    lax.fori_loop(1, 8, greet_z, 0)
    pl.semaphore_wait(barrier, 23)

    first = send(x_ref.at[1 - core], from_core, send_sems.at[0], recv_sems.at[0], partner)
    first.start()
    first.wait_recv()
    half[...] = x_ref[core] + from_core[...]

    def to_plane(p, carry):
        qd = lax.rem(q + p, 16)
        send(half.at[qd], from_plane.at[p - 1], send_sems.at[1], recv_sems.at[1], device_at(core, z, qd)).start()
        return carry

    lax.fori_loop(1, 16, to_plane, 0)
    wait_for(from_plane, recv_sems.at[1])
    part[...] = half[q] + jnp.sum(from_plane[...], axis=0)

    def to_z(p, carry):
        zd = lax.rem(z + p, 8)
        send(part.at[zd], from_z.at[p - 1], send_sems.at[2], recv_sems.at[2], device_at(core, zd, q)).start()
        return carry

    lax.fori_loop(1, 8, to_z, 0)
    wait_for(from_z, recv_sems.at[2])
    piece[...] = (part[z] + jnp.sum(from_z[...], axis=0)) * scale

    def back_z(p, carry):
        send(piece, all_z.at[z], send_sems.at[3], recv_sems.at[3], device_at(core, lax.rem(z + p, 8), q)).start()
        return carry

    lax.fori_loop(1, 8, back_z, 0)
    all_z[z] = piece[...]
    wait_for(from_z, recv_sems.at[3])

    def back_plane(p, carry):
        send(all_z, all_plane.at[q], send_sems.at[4], recv_sems.at[4], device_at(core, z, lax.rem(q + p, 16))).start()
        return carry

    lax.fori_loop(1, 16, back_plane, 0)
    all_plane[q] = all_z[...]
    wait_for(from_plane, recv_sems.at[4])
    last = send(all_plane, all_core, send_sems.at[5], recv_sems.at[5], partner)
    last.start()
    o_ref[core] = all_plane[...]
    last.wait_recv()
    o_ref[1 - core] = all_core[...]
    first.wait_send()
    wait_for(from_plane, send_sems.at[1])
    wait_for(from_z, send_sems.at[2])
    wait_for(from_z, send_sems.at[3])
    wait_for(from_plane, send_sems.at[4])
    last.wait_send()


def reduce_all(x, scale, lanes):
    unit = (8, lanes)
    return pl.pallas_call(
        functools.partial(reduce_kernel, scale),
        out_shape=jax.ShapeDtypeStruct((2, 16, 8) + unit, F32),
        in_specs=[pl.BlockSpec(memory_space=pltpu.VMEM)],
        out_specs=pl.BlockSpec(memory_space=pltpu.VMEM),
        scratch_shapes=[
            pltpu.VMEM((16, 8) + unit, F32),
            pltpu.VMEM((15, 8) + unit, F32),
            pltpu.VMEM((7,) + unit, F32),
            pltpu.VMEM((16, 8) + unit, F32),
            pltpu.VMEM((8,) + unit, F32),
            pltpu.VMEM(unit, F32),
            pltpu.VMEM((8,) + unit, F32),
            pltpu.VMEM((16, 8) + unit, F32),
            pltpu.VMEM((16, 8) + unit, F32),
            pltpu.SemaphoreType.DMA((6,)),
            pltpu.SemaphoreType.DMA((6,)),
        ],
        compiler_params=pltpu.CompilerParams(collective_id=0, has_side_effects=True),
        name="reduce_all",
    )(x)


def to_tiles(a):
    return a.reshape(a.shape[0] // 8, 8, a.shape[1] // 128, 128).transpose(0, 2, 1, 3).reshape(-1, 8, 128)


def from_tiles(t, shape):
    return t.reshape(shape[0] // 8, shape[1] // 128, 8, 128).transpose(0, 2, 1, 3).reshape(shape)


def sum_everywhere(arrays, gain_all, bias_all, scale):
    tiles = [to_tiles(a) for a in arrays]
    small = jnp.concatenate([gain_all, bias_all, jnp.zeros((2, 128), F32)], axis=0)[None]
    used = sum(t.shape[0] for t in tiles) + 1
    joined = jnp.concatenate(tiles + [small, jnp.zeros((256 - used, 8, 128), F32)], axis=0)
    total = reduce_all(joined.reshape(2, 16, 8, 8, 128), scale, 128).reshape(256, 8, 128)
    outs, at = [], 0
    for a, t in zip(arrays, tiles):
        outs.append(from_tiles(total[at : at + t.shape[0]], a.shape))
        at += t.shape[0]
    return outs, total[at, 0:3], total[at, 3:6]


def for_sending(x):
    return jax.tree.map(lambda a: a.astype(jnp.bfloat16) if a.dtype == jnp.float32 else a, x)


def contract(pattern, left_side, right_side):
    return jnp.einsum(pattern, left_side, right_side, preferred_element_type=jnp.float32)


def norm_forward(values, gain_vec, bias_vec, norm_axis):
    center = values - jnp.mean(values, axis=norm_axis, keepdims=True)
    inv_std = lax.rsqrt(jnp.mean(center * center, axis=norm_axis, keepdims=True) + EPSILON)
    normed = center * inv_std
    return (normed, inv_std, normed * gain_vec + bias_vec)


def norm_backward(upstream, normed, inv_std, gain_vec, norm_axis, others):
    grad_gain = jnp.sum(upstream * normed, axis=others)
    grad_bias = jnp.sum(upstream, axis=others)
    scaled = upstream * gain_vec
    result = inv_std * (
        scaled
        - jnp.mean(scaled, axis=norm_axis, keepdims=True)
        - normed * jnp.mean(scaled * normed, axis=norm_axis, keepdims=True)
    )
    return (result, grad_gain, grad_bias)


def enter_rows(pair_rows, row_keep, col_keep, proj_weight, norm_gain, norm_bias):
    channels = pair_rows.shape[2]
    normed_in, inv_in, scaled_in = norm_forward(
        pair_rows.astype(jnp.float32), norm_gain[0], norm_bias[0], 2
    )
    input_bf = scaled_in.astype(jnp.bfloat16)
    factor_pre = contract("rld,de->erl", input_bf, proj_weight[:, : 4 * channels])
    gate_pre = contract("rld,de->rle", input_bf, proj_weight[:, 4 * channels :])
    keep_both = row_keep[:, None] * col_keep[None, :]
    left_bf = (
        jax.nn.sigmoid(factor_pre[:channels]) * factor_pre[channels : 2 * channels] * keep_both
    ).astype(jnp.bfloat16)
    right_bf = (
        jax.nn.sigmoid(factor_pre[2 * channels : 3 * channels])
        * factor_pre[3 * channels :]
        * keep_both
    ).astype(jnp.bfloat16)
    return (input_bf, normed_in, inv_in, factor_pre, gate_pre, keep_both, left_bf, right_bf)


def middle_rows(
    pair_rows,
    cot_rows,
    product_bf,
    gate_pre,
    out_weight,
    up_weight,
    down_weight,
    norm_gain,
    norm_bias,
):
    prod_normed, prod_inv, prod_scaled = norm_forward(
        product_bf.astype(jnp.float32), norm_gain[1][:, None, None], norm_bias[1][:, None, None], 0
    )
    prod_norm_bf = prod_scaled.astype(jnp.bfloat16)
    update = contract("crj,cd->rjd", prod_norm_bf, out_weight)
    gate_sig = jax.nn.sigmoid(gate_pre)
    first_bf = (pair_rows.astype(jnp.float32) + gate_sig * update).astype(jnp.bfloat16)
    tran_normed, tran_inv, tran_scaled = norm_forward(
        first_bf.astype(jnp.float32), norm_gain[2], norm_bias[2], 2
    )
    tran_bf = tran_scaled.astype(jnp.bfloat16)
    hidden_pre = contract("rld,dh->rlh", tran_bf, up_weight)
    hidden_sig = jax.nn.sigmoid(hidden_pre)
    hidden_bf = (hidden_pre * hidden_sig).astype(jnp.bfloat16)
    grad_down = contract("rlh,rld->hd", hidden_bf, cot_rows)
    hidden_grad_bf = (
        contract("rld,hd->rlh", cot_rows, down_weight)
        * hidden_sig
        * (1.0 + hidden_pre * (1.0 - hidden_sig))
    ).astype(jnp.bfloat16)
    grad_up = contract("rld,rlh->dh", tran_bf, hidden_grad_bf)
    tran_grad = contract("rlh,dh->rld", hidden_grad_bf, up_weight)
    first_grad, gain_tran, bias_tran = norm_backward(
        tran_grad, tran_normed, tran_inv, norm_gain[2], 2, (0, 1)
    )
    first_grad = first_grad + cot_rows.astype(jnp.float32)
    update_grad_bf = (first_grad * gate_sig).astype(jnp.bfloat16)
    gate_grad_bf = (first_grad * update * gate_sig * (1.0 - gate_sig)).astype(jnp.bfloat16)
    grad_out = contract("crj,rjd->cd", prod_norm_bf, update_grad_bf)
    norm_grad = contract("rjd,cd->crj", update_grad_bf, out_weight)
    prod_grad, gain_prod, bias_prod = norm_backward(
        norm_grad, prod_normed, prod_inv, norm_gain[1][:, None, None], 0, (1, 2)
    )
    return (
        prod_grad.astype(jnp.bfloat16),
        first_grad,
        gate_grad_bf,
        grad_out,
        grad_up,
        grad_down,
        gain_prod,
        bias_prod,
        gain_tran,
        bias_tran,
    )


def leave_rows(
    left_grad,
    right_grad,
    factor_pre,
    keep_both,
    gate_grad_bf,
    input_bf,
    normed_in,
    inv_in,
    first_grad,
    proj_weight,
    norm_gain,
):
    channels = gate_grad_bf.shape[2]
    sig_left = jax.nn.sigmoid(factor_pre[:channels])
    lin_left = factor_pre[channels : 2 * channels]
    sig_right = jax.nn.sigmoid(factor_pre[2 * channels : 3 * channels])
    lin_right = factor_pre[3 * channels :]
    masked_left = left_grad.astype(jnp.float32) * keep_both
    masked_right = right_grad.astype(jnp.float32) * keep_both
    factor_grad = jnp.concatenate(
        [
            masked_left * lin_left * sig_left * (1.0 - sig_left),
            masked_left * sig_left,
            masked_right * lin_right * sig_right * (1.0 - sig_right),
            masked_right * sig_right,
        ],
        axis=0,
    ).astype(jnp.bfloat16)
    grad_proj = jnp.concatenate(
        [
            contract("rld,erl->de", input_bf, factor_grad),
            contract("rld,rle->de", input_bf, gate_grad_bf),
        ],
        axis=1,
    )
    input_grad = contract("erl,de->rld", factor_grad, proj_weight[:, : 4 * channels]) + contract(
        "rle,de->rld", gate_grad_bf, proj_weight[:, 4 * channels :]
    )
    pair_grad, gain_in, bias_in = norm_backward(
        input_grad, normed_in, inv_in, norm_gain[0], 2, (0, 1)
    )
    return ((pair_grad + first_grad).astype(jnp.bfloat16), grad_proj, gain_in, bias_in)


def channel_products(left_part, right_part):
    return contract("acik,acjk->acij", left_part, right_part).astype(jnp.bfloat16)


def channel_grads(grad_part, left_part, right_part):
    left_grad = contract("acij,acjk->acik", grad_part, right_part).astype(jnp.bfloat16)
    right_grad = contract("acij,acik->acjk", grad_part, left_part).astype(jnp.bfloat16)
    return (left_grad, right_grad)


def local(
    pair, cotangent, lengths, proj_weight, out_weight, up_weight, down_weight, norm_gain, norm_bias
):
    pair_rows = pair[0]
    cot_rows = cotangent[0]
    rows_here, length_all, channels = pair_rows.shape
    groups = lax.axis_size("row")
    per_group = channels // groups
    first_row = lax.axis_index("row") * rows_here
    row_keep = (first_row + jnp.arange(rows_here, dtype=jnp.int32) < lengths[0]).astype(jnp.float32)
    col_keep = (jnp.arange(length_all, dtype=jnp.int32) < lengths[0]).astype(jnp.float32)
    entered = enter_rows(pair_rows, row_keep, col_keep, proj_weight, norm_gain, norm_bias)
    input_bf, normed_in, inv_in, factor_pre, gate_pre, keep_both, left_bf, right_bf = entered
    left_split = left_bf.reshape(groups, per_group, rows_here, length_all)
    right_split = right_bf.reshape(groups, per_group, rows_here, length_all)
    left_owned, right_owned = side_by_side((left_split, right_split), "row", 0, 2, 1)
    product_owned = channel_products(left_owned, right_owned)
    product_split = lax.all_to_all(product_owned, "row", split_axis=2, concat_axis=0, tiled=True)
    product_bf = product_split.reshape(channels, rows_here, length_all)
    middle = middle_rows(
        pair_rows,
        cot_rows,
        product_bf,
        gate_pre,
        out_weight,
        up_weight,
        down_weight,
        norm_gain,
        norm_bias,
    )
    (
        prod_grad_bf,
        first_grad,
        gate_grad_bf,
        grad_out,
        grad_up,
        grad_down,
        gain_prod,
        bias_prod,
        gain_tran,
        bias_tran,
    ) = middle
    grad_split = prod_grad_bf.reshape(groups, per_group, rows_here, length_all)
    grad_owned = lax.all_to_all(grad_split, "row", split_axis=0, concat_axis=2, tiled=True)
    left_home, right_home = lax.all_to_all(
        for_sending(channel_grads(grad_owned, left_owned, right_owned)),
        "row",
        split_axis=2,
        concat_axis=0,
        tiled=True,
    )
    left_grad = left_home.reshape(channels, rows_here, length_all)
    right_grad = right_home.reshape(channels, rows_here, length_all)
    pair_grad, grad_proj, gain_in, bias_in = leave_rows(
        left_grad,
        right_grad,
        factor_pre,
        keep_both,
        gate_grad_bf,
        input_bf,
        normed_in,
        inv_in,
        first_grad,
        proj_weight,
        norm_gain,
    )
    gain_all = jnp.stack([gain_in, gain_prod, gain_tran])
    bias_all = jnp.stack([bias_in, bias_prod, bias_tran])
    factor = 1.0 / (rows_here * groups)
    sums, summed_gain, summed_bias = sum_everywhere(
        (grad_proj, grad_out, grad_up, grad_down), gain_all, bias_all, factor
    )
    return (pair_grad[None], *sums, summed_gain, summed_bias)


def solution(mesh):
    in_specs = (
        P("crop", "row", None, None),
        P("crop", "row", None, None),
        P("crop"),
        P(),
        P(),
        P(),
        P(),
        P(),
        P(),
    )
    out_specs = (P("crop", "row", None, None), P(), P(), P(), P(), P(), P())
    return jax.shard_map(local, mesh=mesh, in_specs=in_specs, out_specs=out_specs, check_vma=False)
```

```python
import functools

import jax
import jax.numpy as jnp
from jax import lax
from jax.experimental import pallas as pl
from jax.experimental.pallas import tpu as pltpu
from jax.sharding import PartitionSpec as P

EPSILON = 1e-05
F32 = jnp.float32
BF16 = jnp.bfloat16
MESH = pl.DeviceIdType.MESH
CHUNKS = 4


def place():
    crop = lax.axis_index("crop")
    row = lax.axis_index("row")
    core = lax.rem(crop, 2)
    zhi = lax.div(crop, 2)
    q = lax.div(row, 4)
    zlo = lax.rem(row, 4)
    return core, zhi * 4 + zlo, q


def device_at(core, z, q):
    return (lax.div(z, 4) * 2 + core, q * 4 + lax.rem(z, 4))


def send(src, dst, send_sem, recv_sem, device):
    return pltpu.make_async_remote_copy(
        src_ref=src,
        dst_ref=dst,
        send_sem=send_sem,
        recv_sem=recv_sem,
        device_id=device,
        device_id_type=MESH,
    )


def wait_for(ref, sem):
    pltpu.make_async_copy(ref, ref, sem).wait()


def signal(sem, device):
    pl.semaphore_signal(sem, inc=1, device_id=device, device_id_type=MESH)


def looped(count, body):
    lax.fori_loop(0, count, lambda i, carry: (body(i), carry)[1], 0)


def peers(body):
    crop = lax.axis_index("crop")
    row = lax.axis_index("row")
    q = lax.div(row, 4)
    z = lax.rem(row, 4)

    def step(i):
        n = i + 1
        dest = lax.rem(q + lax.rem(n, 16), 16) * 4 + lax.rem(z + lax.div(n, 16), 4)
        body(dest, (crop, dest))

    looped(63, step)


def sigmoid(x):
    return 0.5 + 0.5 * jnp.tanh(0.5 * x)


def dot(a, b, dim_a, dim_b):
    return lax.dot_general(a, b, (((dim_a,), (dim_b,)), ((), ())), preferred_element_type=F32)


def norm(values, axis):
    center = values - jnp.mean(values, axis=axis, keepdims=True)
    inv_std = lax.rsqrt(jnp.mean(center * center, axis=axis, keepdims=True) + EPSILON)
    return center * inv_std, inv_std


def norm_back(upstream, normed, inv_std, gain, axis):
    scaled = upstream * gain
    return inv_std * (
        scaled
        - jnp.mean(scaled, axis=axis, keepdims=True)
        - normed * jnp.mean(scaled * normed, axis=axis, keepdims=True)
    )


def to_flat(turn, value):
    turn[...] = value.reshape(1024, 128)
    return jnp.concatenate([turn[pl.ds(r, 128, stride=8), :] for r in range(8)], axis=1)


def to_rows(turn, value):
    for r in range(8):
        turn[pl.ds(r, 128, stride=8), :] = value[:, r * 128 : (r + 1) * 128]
    return turn[...].reshape(128, 8, 128)


def column(j):
    return pl.ds(pl.multiple_of(j * 128, 128), 128)


def whole_kernel(
    scale,
    pair_ref,
    cot_ref,
    keep_ref,
    wt_ref,
    wg_ref,
    out_ref,
    up_ref,
    down_ref,
    vec_ref,
    gain1_ref,
    bias1_ref,
    grad_ref,
    sums_ref,
    factors_out,
    factors_in,
    left_mat,
    right_mat,
    prod_out,
    prod_in,
    cots_out,
    cots_in,
    grads_out,
    grads_in,
    turn_a,
    turn_b,
    first_ref,
    gate_ref,
    acc,
    columns,
    from_core,
    from_plane,
    from_z,
    half,
    part,
    piece,
    all_z,
    all_plane,
    all_core,
    xs,
    xr,
    send_sems,
    recv_sems,
):
    core, z8, q = place()
    row = lax.axis_index("row")
    partner = device_at(1 - core, z8, q)
    barrier = pltpu.get_barrier_semaphore()
    signal(barrier, partner)
    peers(lambda dest, device: signal(barrier, device))
    looped(4, lambda i: signal(barrier, device_at(core, lax.rem(lax.div(z8, 4) * 4 + 4 + i, 8), q)))
    acc[...] = jnp.zeros_like(acc)
    columns[...] = jnp.zeros_like(columns)
    gain0, bias0 = vec_ref[0:1], vec_ref[1:2]
    gain2, bias2 = vec_ref[2:3], vec_ref[3:4]

    def rows_of(ref, j):
        return ref[:, column(j), :].reshape(1024, 128)

    def enter(j):
        normed, inv = norm(rows_of(pair_ref, j).astype(F32), 1)
        entered = (normed * gain0 + bias0).astype(BF16)
        return normed, inv, entered

    def enter_chunk(j):
        _, _, entered = enter(j)
        keep = keep_ref[j]
        pre = dot(wt_ref[...], entered, 1, 1)
        left = sigmoid(pre[0:128]) * pre[128:256] * keep
        right = sigmoid(pre[256:384]) * pre[384:512] * keep
        factors_out[:, 0, :, :, column(j)] = to_rows(turn_a, left).astype(BF16).reshape(64, 2, 8, 128)
        factors_out[:, 1, :, :, column(j)] = to_rows(turn_b, right).astype(BF16).reshape(64, 2, 8, 128)

    looped(CHUNKS, enter_chunk)
    pl.semaphore_wait(barrier, 68)

    def exchange(n, src, dst):
        def one(dest, device):
            send(src.at[dest], dst.at[row], xs.at[n], xr.at[n], device).start()

        peers(one)
        dst[row] = src[row]
        wait_for(dst.at[pl.ds(0, 63)], xr.at[n])

    exchange(0, factors_out, factors_in)

    def matrix(value):
        return value.astype(F32).reshape(512, 512).astype(BF16)

    def product(c):
        left_mat[c] = matrix(factors_in[:, 0, c])
        right_mat[c] = matrix(factors_in[:, 1, c])
        prod_out[:, c] = dot(left_mat[c], right_mat[c], 1, 1).reshape(64, 8, 512).astype(BF16)

    looped(2, product)
    exchange(1, prod_out, prod_in)

    def middle(j):
        flat = to_flat(turn_a, prod_in[:, :, :, column(j)].astype(F32))
        gain1 = gain1_ref[...]
        prod_normed, prod_inv = norm(flat, 0)
        prod_bf = (prod_normed * gain1 + bias1_ref[...]).astype(BF16)
        update = dot(prod_bf, out_ref[...], 0, 0)
        _, _, entered = enter(j)
        gate = sigmoid(dot(entered, wg_ref[...], 1, 0))
        first = (rows_of(pair_ref, j).astype(F32) + gate * update).astype(BF16)
        tran_normed, tran_inv = norm(first.astype(F32), 1)
        tran_bf = (tran_normed * gain2 + bias2).astype(BF16)
        cot = rows_of(cot_ref, j)
        tran_grad = jnp.zeros((1024, 128), F32)
        for h in range(2):
            at = slice(h * 256, (h + 1) * 256)
            hidden_pre = dot(tran_bf, up_ref[:, at], 1, 0)
            hidden_sig = sigmoid(hidden_pre)
            hidden = (hidden_pre * hidden_sig).astype(BF16)
            acc[h * 256 : (h + 1) * 256] += dot(hidden, cot, 0, 0)
            hidden_grad = (
                dot(cot, down_ref[at, :], 1, 1)
                * hidden_sig
                * (1.0 + hidden_pre * (1.0 - hidden_sig))
            ).astype(BF16)
            acc[512 + h * 256 : 512 + (h + 1) * 256] += dot(hidden_grad, tran_bf, 0, 0)
            tran_grad += dot(hidden_grad, up_ref[:, at], 1, 1)
        acc[1802:1803] += jnp.sum(tran_grad * tran_normed, axis=0, keepdims=True)
        acc[1805:1806] += jnp.sum(tran_grad, axis=0, keepdims=True)
        first_grad = norm_back(tran_grad, tran_normed, tran_inv, gain2, 1) + cot.astype(F32)
        update_grad = (first_grad * gate).astype(BF16)
        gate_grad = (first_grad * update * gate * (1.0 - gate)).astype(BF16)
        first_ref[:, column(j), :] = first_grad.reshape(8, 128, 128)
        gate_ref[:, column(j), :] = gate_grad.reshape(8, 128, 128)
        acc[1024:1152] += dot(prod_bf, update_grad, 1, 0)
        norm_grad = dot(out_ref[...], update_grad, 1, 1)
        columns[:, 0:1] += jnp.sum(norm_grad * prod_normed, axis=1, keepdims=True)
        columns[:, 1:2] += jnp.sum(norm_grad, axis=1, keepdims=True)
        prod_grad = norm_back(norm_grad, prod_normed, prod_inv, gain1, 0)
        cots_out[:, :, :, column(j)] = to_rows(turn_b, prod_grad).astype(BF16).reshape(64, 2, 8, 128)

    looped(CHUNKS, middle)
    exchange(2, cots_out, cots_in)

    def product_grads(c):
        grad = matrix(cots_in[:, c])
        grads_out[:, 0, c] = dot(grad, right_mat[c], 1, 0).reshape(64, 8, 512).astype(BF16)
        grads_out[:, 1, c] = dot(grad, left_mat[c], 0, 0).reshape(64, 8, 512).astype(BF16)

    looped(2, product_grads)
    exchange(3, grads_out, grads_in)

    def leave(j):
        normed, inv, entered = enter(j)
        keep = keep_ref[j]
        pre = dot(wt_ref[...], entered, 1, 1)
        left = to_flat(turn_a, grads_in[:, 0, :, :, column(j)].astype(F32)) * keep
        right = to_flat(turn_b, grads_in[:, 1, :, :, column(j)].astype(F32)) * keep
        left_sig = sigmoid(pre[0:128])
        right_sig = sigmoid(pre[256:384])
        factor_grad = jnp.concatenate(
            [
                (left * pre[128:256] * left_sig * (1.0 - left_sig)).astype(BF16),
                (left * left_sig).astype(BF16),
                (right * pre[384:512] * right_sig * (1.0 - right_sig)).astype(BF16),
                (right * right_sig).astype(BF16),
            ],
            axis=0,
        )
        gate_grad = rows_of(gate_ref, j)
        acc[1152:1664] += dot(factor_grad, entered, 1, 0)
        acc[1664:1792] += dot(gate_grad, entered, 0, 0)
        input_grad = dot(factor_grad, wt_ref[...], 0, 0) + dot(gate_grad, wg_ref[...], 1, 1)
        acc[1800:1801] += jnp.sum(input_grad * normed, axis=0, keepdims=True)
        acc[1803:1804] += jnp.sum(input_grad, axis=0, keepdims=True)
        result = norm_back(input_grad, normed, inv, gain0, 1) + rows_of(first_ref, j)
        grad_ref[:, column(j), :] = result.astype(BF16).reshape(8, 128, 128)

    looped(CHUNKS, leave)
    turned = columns[...].T
    acc[1801:1802] = turned[0:1]
    acc[1804:1805] = turned[1:2]

    def rows(i, count):
        return pl.ds(pl.multiple_of(i * count, count), count)

    first = send(acc.at[rows(1 - core, 1024)], from_core, send_sems.at[0], recv_sems.at[0], partner)
    first.start()
    first.wait_recv()
    half[...] = acc[rows(core, 1024)] + from_core[...]

    def to_plane(i):
        qd = lax.rem(q + i + 1, 16)
        send(half.at[rows(qd, 64)], from_plane.at[i], send_sems.at[1], recv_sems.at[1], device_at(core, z8, qd)).start()

    looped(15, to_plane)
    wait_for(from_plane, recv_sems.at[1])
    part[...] = half[rows(q, 64)] + jnp.sum(from_plane[...], axis=0)

    def to_z(i):
        zd = lax.rem(z8 + i + 1, 8)
        send(part.at[rows(zd, 8)], from_z.at[i], send_sems.at[2], recv_sems.at[2], device_at(core, zd, q)).start()

    looped(7, to_z)
    wait_for(from_z, recv_sems.at[2])
    piece[...] = (part[rows(z8, 8)] + jnp.sum(from_z[...], axis=0)) * scale

    def back_z(i):
        send(piece, all_z.at[rows(z8, 8)], send_sems.at[3], recv_sems.at[3], device_at(core, lax.rem(z8 + i + 1, 8), q)).start()

    looped(7, back_z)
    all_z[rows(z8, 8)] = piece[...]
    wait_for(from_z, recv_sems.at[3])

    def back_plane(i):
        send(all_z, all_plane.at[rows(q, 64)], send_sems.at[4], recv_sems.at[4], device_at(core, z8, lax.rem(q + i + 1, 16))).start()

    looped(15, back_plane)
    all_plane[rows(q, 64)] = all_z[...]
    wait_for(from_plane, recv_sems.at[4])
    last = send(all_plane, all_core, send_sems.at[5], recv_sems.at[5], partner)
    last.start()
    sums_ref[rows(core, 1024)] = all_plane[...]
    last.wait_recv()
    sums_ref[rows(1 - core, 1024)] = all_core[...]
    first.wait_send()
    wait_for(from_plane, send_sems.at[1])
    wait_for(from_z, send_sems.at[2])
    wait_for(from_z, send_sems.at[3])
    wait_for(from_plane, send_sems.at[4])
    last.wait_send()
    wait_for(factors_in.at[pl.ds(0, 63)], xs.at[0])
    wait_for(prod_in.at[pl.ds(0, 63)], xs.at[1])
    wait_for(cots_in.at[pl.ds(0, 63)], xs.at[2])
    wait_for(grads_in.at[pl.ds(0, 63)], xs.at[3])


def local(
    pair, cotangent, lengths, proj_weight, out_weight, up_weight, down_weight, norm_gain, norm_bias
):
    pair_rows = pair[0]
    cot_rows = cotangent[0]
    rows_here, length_all, channels = pair_rows.shape
    wide = 4 * channels
    first_row = lax.axis_index("row") * rows_here
    row_keep = (first_row + jnp.arange(rows_here, dtype=jnp.int32) < lengths[0]).astype(F32)
    col_keep = (jnp.arange(length_all, dtype=jnp.int32) < lengths[0]).astype(F32)
    keep = (row_keep[None, :, None] * col_keep.reshape(CHUNKS, 1, 128)).reshape(CHUNKS, 1, 1024)
    vec = jnp.concatenate(
        [norm_gain[0:1], norm_bias[0:1], norm_gain[2:3], norm_bias[2:3], jnp.zeros((4, channels), F32)]
    )
    vmem = pl.BlockSpec(memory_space=pltpu.VMEM)
    both = (64, 2, 2, 8, 512)
    single = (64, 2, 8, 512)
    pair_grad, sums = pl.pallas_call(
        functools.partial(whole_kernel, 1.0 / length_all),
        out_shape=(
            jax.ShapeDtypeStruct(pair_rows.shape, BF16),
            jax.ShapeDtypeStruct((2048, 128), F32),
        ),
        in_specs=[vmem] * 11,
        out_specs=(vmem, vmem),
        scratch_shapes=[
            pltpu.VMEM(both, BF16),
            pltpu.VMEM(both, BF16),
            pltpu.VMEM((2, 512, 512), BF16),
            pltpu.VMEM((2, 512, 512), BF16),
            pltpu.VMEM(single, BF16),
            pltpu.VMEM(single, BF16),
            pltpu.VMEM(single, BF16),
            pltpu.VMEM(single, BF16),
            pltpu.VMEM(both, BF16),
            pltpu.VMEM(both, BF16),
            pltpu.VMEM((1024, 128), F32),
            pltpu.VMEM((1024, 128), F32),
            pltpu.VMEM(pair_rows.shape, F32),
            pltpu.VMEM(pair_rows.shape, BF16),
            pltpu.VMEM((2048, 128), F32),
            pltpu.VMEM((128, 128), F32),
            pltpu.VMEM((1024, 128), F32),
            pltpu.VMEM((15, 64, 128), F32),
            pltpu.VMEM((7, 8, 128), F32),
            pltpu.VMEM((1024, 128), F32),
            pltpu.VMEM((64, 128), F32),
            pltpu.VMEM((8, 128), F32),
            pltpu.VMEM((64, 128), F32),
            pltpu.VMEM((1024, 128), F32),
            pltpu.VMEM((1024, 128), F32),
            pltpu.SemaphoreType.DMA((4,)),
            pltpu.SemaphoreType.DMA((4,)),
            pltpu.SemaphoreType.DMA((6,)),
            pltpu.SemaphoreType.DMA((6,)),
        ],
        compiler_params=pltpu.CompilerParams(
            collective_id=0, has_side_effects=True, vmem_limit_bytes=60 * 1024 * 1024
        ),
        name="whole",
    )(
        pair_rows,
        cot_rows,
        keep,
        proj_weight[:, :wide].T,
        proj_weight[:, wide:],
        out_weight,
        up_weight,
        down_weight,
        vec,
        norm_gain[1][:, None],
        norm_bias[1][:, None],
    )
    return (
        pair_grad[None],
        sums[1152:1792].T,
        sums[1024:1152],
        sums[512:1024].T,
        sums[0:512],
        sums[1800:1803],
        sums[1803:1806],
    )


def solution(mesh):
    in_specs = (
        P("crop", "row", None, None),
        P("crop", "row", None, None),
        P("crop"),
        P(),
        P(),
        P(),
        P(),
        P(),
        P(),
    )
    out_specs = (P("crop", "row", None, None), P(), P(), P(), P(), P(), P())
    return jax.shard_map(local, mesh=mesh, in_specs=in_specs, out_specs=out_specs, check_vma=False)
```

```python
import functools

import jax
import jax.numpy as jnp
from jax import lax
from jax.experimental import pallas as pl
from jax.experimental.pallas import tpu as pltpu
from jax.sharding import PartitionSpec as P

EPSILON = 1e-05
F32 = jnp.float32
BF16 = jnp.bfloat16
MESH = pl.DeviceIdType.MESH
CHUNKS = 4


def place():
    crop = lax.axis_index("crop")
    row = lax.axis_index("row")
    core = lax.rem(crop, 2)
    zhi = lax.div(crop, 2)
    q = lax.div(row, 4)
    zlo = lax.rem(row, 4)
    return core, zhi * 4 + zlo, q


def device_at(core, z, q):
    return (lax.div(z, 4) * 2 + core, q * 4 + lax.rem(z, 4))


def send(src, dst, send_sem, recv_sem, device):
    return pltpu.make_async_remote_copy(
        src_ref=src,
        dst_ref=dst,
        send_sem=send_sem,
        recv_sem=recv_sem,
        device_id=device,
        device_id_type=MESH,
    )


def wait_for(ref, sem):
    pltpu.make_async_copy(ref, ref, sem).wait()


def signal(sem, device):
    pl.semaphore_signal(sem, inc=1, device_id=device, device_id_type=MESH)


def looped(count, body):
    lax.fori_loop(0, count, lambda i, carry: (body(i), carry)[1], 0)


def peers(body):
    crop = lax.axis_index("crop")
    row = lax.axis_index("row")
    q = lax.div(row, 4)
    z = lax.rem(row, 4)

    def step(i):
        n = i + 1
        dest = lax.rem(q + lax.rem(n, 16), 16) * 4 + lax.rem(z + lax.div(n, 16), 4)
        body(dest, (crop, dest))

    looped(63, step)


def sigmoid(x):
    return 0.5 + 0.5 * jnp.tanh(0.5 * x)


def dot(a, b, dim_a, dim_b):
    return lax.dot_general(a, b, (((dim_a,), (dim_b,)), ((), ())), preferred_element_type=F32)


def norm(values, axis):
    center = values - jnp.mean(values, axis=axis, keepdims=True)
    inv_std = lax.rsqrt(jnp.mean(center * center, axis=axis, keepdims=True) + EPSILON)
    return center * inv_std, inv_std


def norm_back(upstream, normed, inv_std, gain, axis):
    scaled = upstream * gain
    return inv_std * (
        scaled
        - jnp.mean(scaled, axis=axis, keepdims=True)
        - normed * jnp.mean(scaled * normed, axis=axis, keepdims=True)
    )


def to_flat(turn, value):
    turn[...] = value.reshape(1024, 128)
    return jnp.concatenate([turn[pl.ds(r, 128, stride=8), :] for r in range(8)], axis=1)


def to_rows(turn, value):
    for r in range(8):
        turn[pl.ds(r, 128, stride=8), :] = value[:, r * 128 : (r + 1) * 128]
    return turn[...].reshape(128, 8, 128)


def column(j):
    return pl.ds(pl.multiple_of(j * 128, 128), 128)


def place_of(ref, j):
    return ref[:, column(j), :].reshape(1024, 128)


def rows(i, count):
    return pl.ds(pl.multiple_of(i * count, count), count)


def block(b):
    return slice(b * 128, (b + 1) * 128)


def whole_kernel(
    scale,
    lengths_ref,
    pair_ref,
    cot_ref,
    proj_ref,
    out_ref,
    up_ref,
    down_ref,
    gain_ref,
    bias_ref,
    grad_ref,
    sum_proj,
    sum_out,
    sum_up,
    sum_down,
    sum_gain,
    sum_bias,
    factors_out,
    factors_in,
    left_mat,
    right_mat,
    prod_out,
    prod_in,
    cots_out,
    cots_in,
    cot_mat,
    cot_turned,
    grads_out,
    grads_in,
    turn_a,
    turn_b,
    wt_ref,
    gain_col,
    bias_col,
    first_ref,
    gate_ref,
    acc,
    tail,
    columns,
    from_core,
    from_plane,
    from_z,
    half,
    part,
    piece,
    all_z,
    all_plane,
    all_core,
    acc_sum,
    tail_core,
    tail_half,
    tail_plane,
    tail_part,
    tail_z,
    tail_piece,
    tail_all,
    tail_other,
    xs,
    xr,
    send_sems,
    recv_sems,
):
    core, z8, q = place()
    row = lax.axis_index("row")
    partner = device_at(1 - core, z8, q)
    barrier = pltpu.get_barrier_semaphore()
    signal(barrier, partner)
    peers(lambda dest, device: signal(barrier, device))
    looped(4, lambda i: signal(barrier, device_at(core, lax.rem(lax.div(z8, 4) * 4 + 4 + i, 8), q)))
    acc[...] = jnp.zeros_like(acc)
    tail[...] = jnp.zeros_like(tail)
    columns[...] = jnp.zeros_like(columns)
    for b in range(4):
        wt_ref[block(b)] = proj_ref[:, block(b)].T
    gain_col[...] = jnp.broadcast_to(gain_ref[1:2], (128, 128)).T
    bias_col[...] = jnp.broadcast_to(bias_ref[1:2], (128, 128)).T
    gain0, bias0 = gain_ref[0:1], bias_ref[0:1]
    gain2, bias2 = gain_ref[2:3], bias_ref[2:3]
    gate_weight = slice(512, 640)

    def enter(j):
        normed, inv = norm(place_of(pair_ref, j).astype(F32), 1)
        entered = (normed * gain0 + bias0).astype(BF16)
        return normed, inv, entered

    def keep_of(j):
        at = lax.broadcasted_iota(jnp.int32, (1, 1024), 1)
        row_at = row * 8 + lax.shift_right_logical(at, 7)
        col_at = j * 128 + jnp.bitwise_and(at, 127)
        return jnp.where(jnp.maximum(row_at, col_at) < lengths_ref[0], 1.0, 0.0)

    def start_chunk(n, j, src, dst):
        def one(dest, device):
            send(src.at[j, dest], dst.at[j, row], xs.at[n, j], xr.at[n, j], device).start()

        peers(one)
        dst[j, row] = src[j, row]

    def wait_chunk(n, j, dst):
        wait_for(dst.at[j, pl.ds(0, 63)], xr.at[n, j])

    def enter_chunk(j):
        _, _, entered = enter(j)
        keep = keep_of(j)
        pre = dot(wt_ref[...], entered, 1, 1)
        left = sigmoid(pre[0:128]) * pre[128:256] * keep
        right = sigmoid(pre[256:384]) * pre[384:512] * keep
        factors_out[j, :, 0] = to_rows(turn_a, left).astype(BF16).reshape(64, 2, 8, 128)
        factors_out[j, :, 1] = to_rows(turn_b, right).astype(BF16).reshape(64, 2, 8, 128)

        @pl.when(j == 0)
        def _():
            pl.semaphore_wait(barrier, 68)

        start_chunk(0, j, factors_out, factors_in)

    looped(CHUNKS, enter_chunk)

    def matrix(value):
        return value.astype(F32).reshape(512, 128)

    def gather_factors(j):
        wait_chunk(0, j, factors_in)
        for c in range(2):
            left_mat[c, :, column(j)] = matrix(factors_in[j, :, 0, c]).astype(BF16)
            right_mat[c, :, column(j)] = matrix(factors_in[j, :, 1, c]).astype(BF16)

    looped(CHUNKS, gather_factors)

    def product(j):
        for c in range(2):
            prod = dot(left_mat[c], right_mat[c, rows(j, 128), :], 1, 1)
            prod_out[j, :, c] = prod.reshape(64, 8, 128).astype(BF16)
        start_chunk(1, j, prod_out, prod_in)

    looped(CHUNKS, product)

    def middle(j):
        _, _, entered = enter(j)
        gate = sigmoid(dot(entered, proj_ref[:, gate_weight], 1, 0))
        cot = place_of(cot_ref, j)
        cot_t = cot.T
        wait_chunk(1, j, prod_in)
        flat = to_flat(turn_a, prod_in[j].astype(F32))
        gain1 = gain_col[:, 0:1]
        prod_normed, prod_inv = norm(flat, 0)
        prod_bf = (prod_normed * gain1 + bias_col[:, 0:1]).astype(BF16)
        update = dot(prod_bf, out_ref[...], 0, 0)
        first = (place_of(pair_ref, j).astype(F32) + gate * update).astype(BF16)
        tran_normed, tran_inv = norm(first.astype(F32), 1)
        tran_bf = (tran_normed * gain2 + bias2).astype(BF16)
        tran_t = tran_bf.T
        tran_grad = jnp.zeros((1024, 128), F32)
        for h in range(2):
            at = slice(h * 256, (h + 1) * 256)
            hidden_pre = dot(tran_bf, up_ref[:, at], 1, 0)
            hidden_sig = sigmoid(hidden_pre)
            hidden = (hidden_pre * hidden_sig).astype(BF16)
            down_term = dot(cot_t, hidden, 1, 0)
            hidden_grad = (
                dot(cot, down_ref[at, :], 1, 1)
                * hidden_sig
                * (1.0 + hidden_pre * (1.0 - hidden_sig))
            ).astype(BF16)
            up_term = dot(tran_t, hidden_grad, 1, 0)
            for k in range(2):
                acc[block(2 * h + k)] += down_term[:, block(k)]
                acc[block(4 + 2 * h + k)] += up_term[:, block(k)]
            tran_grad += dot(hidden_grad, up_ref[:, at], 1, 1)
        acc[1282:1283] += jnp.sum(tran_grad * tran_normed, axis=0, keepdims=True)
        acc[1285:1286] += jnp.sum(tran_grad, axis=0, keepdims=True)
        first_grad = norm_back(tran_grad, tran_normed, tran_inv, gain2, 1) + cot.astype(F32)
        update_grad = (first_grad * gate).astype(BF16)
        gate_grad = (first_grad * update * gate * (1.0 - gate)).astype(BF16)
        acc[block(8)] += dot(prod_bf, update_grad, 1, 0)
        norm_grad = dot(out_ref[...], update_grad, 1, 1)
        columns[:, 0:1] += jnp.sum(norm_grad * prod_normed, axis=1, keepdims=True)
        columns[:, 1:2] += jnp.sum(norm_grad, axis=1, keepdims=True)
        prod_grad = norm_back(norm_grad, prod_normed, prod_inv, gain1, 0)
        cots_out[j] = to_rows(turn_b, prod_grad).astype(BF16).reshape(64, 2, 8, 128)
        start_chunk(2, j, cots_out, cots_in)
        first_ref[:, column(j), :] = first_grad.reshape(8, 128, 128)
        gate_ref[:, column(j), :] = dot(gate_grad, proj_ref[:, gate_weight], 1, 1).reshape(8, 128, 128)
        acc[block(9)] += dot(entered.T, gate_grad, 1, 0)

    looped(CHUNKS, middle)
    for b in range(4):
        acc[block(b)] = acc[block(b)].T
    turned = columns[...].T
    acc[1281:1282] = turned[0:1]
    acc[1284:1285] = turned[1:2]

    first = send(acc.at[rows(1 - core, 1024)], from_core, send_sems.at[0], recv_sems.at[0], partner)
    first.start()
    first.wait_recv()
    half[...] = acc[rows(core, 1024)] + from_core[...]

    def to_plane(i):
        qd = lax.rem(q + i + 1, 16)
        send(half.at[rows(qd, 64)], from_plane.at[i], send_sems.at[1], recv_sems.at[1], device_at(core, z8, qd)).start()

    looped(15, to_plane)

    def gather_cots(j):
        wait_chunk(2, j, cots_in)
        for c in range(2):
            grad = matrix(cots_in[j, :, c])
            cot_mat[c, :, column(j)] = grad.astype(BF16)
            cot_turned[c, rows(j, 128), :] = grad.T.astype(BF16)

    looped(CHUNKS, gather_cots)
    wait_for(from_plane, recv_sems.at[1])
    part[...] = half[rows(q, 64)] + jnp.sum(from_plane[...], axis=0)

    def to_z(i):
        zd = lax.rem(z8 + i + 1, 8)
        send(part.at[rows(zd, 8)], from_z.at[i], send_sems.at[2], recv_sems.at[2], device_at(core, zd, q)).start()

    looped(7, to_z)

    def product_grads(j):
        for c in range(2):
            left = dot(cot_mat[c], right_mat[c, :, column(j)], 1, 0)
            right = dot(cot_turned[c], left_mat[c, :, column(j)], 1, 0)
            grads_out[j, :, 0, c] = left.reshape(64, 8, 128).astype(BF16)
            grads_out[j, :, 1, c] = right.reshape(64, 8, 128).astype(BF16)
        start_chunk(3, j, grads_out, grads_in)

    looped(CHUNKS, product_grads)
    wait_for(from_z, recv_sems.at[2])
    piece[...] = (part[rows(z8, 8)] + jnp.sum(from_z[...], axis=0)) * scale

    def back_z(i):
        send(piece, all_z.at[rows(z8, 8)], send_sems.at[3], recv_sems.at[3], device_at(core, lax.rem(z8 + i + 1, 8), q)).start()

    looped(7, back_z)
    all_z[rows(z8, 8)] = piece[...]

    def leave(j):
        normed, inv, entered = enter(j)
        keep = keep_of(j)
        pre = dot(wt_ref[...], entered, 1, 1)
        left_sig = sigmoid(pre[0:128])
        right_sig = sigmoid(pre[256:384])
        wait_chunk(3, j, grads_in)
        left = to_flat(turn_a, grads_in[j, :, 0].astype(F32)) * keep
        right = to_flat(turn_b, grads_in[j, :, 1].astype(F32)) * keep
        factor_grad = jnp.concatenate(
            [
                (left * pre[128:256] * left_sig * (1.0 - left_sig)).astype(BF16),
                (left * left_sig).astype(BF16),
                (right * pre[384:512] * right_sig * (1.0 - right_sig)).astype(BF16),
                (right * right_sig).astype(BF16),
            ],
            axis=0,
        )
        terms = dot(factor_grad, entered, 1, 0)
        for core_half in range(2):
            for b in range(16):
                at = core_half * 256 + b * 16
                to = core_half * 384 + b * 24
                tail[to : to + 16] += terms[at : at + 16]
        input_grad = dot(factor_grad, wt_ref[...], 0, 0) + place_of(gate_ref, j)
        tail[16:17] += jnp.sum(input_grad * normed, axis=0, keepdims=True)
        tail[17:18] += jnp.sum(input_grad, axis=0, keepdims=True)
        result = norm_back(input_grad, normed, inv, gain0, 1) + place_of(first_ref, j)
        grad_ref[:, column(j), :] = result.astype(BF16).reshape(8, 128, 128)

    looped(CHUNKS, leave)

    tail_first = send(tail.at[rows(1 - core, 384)], tail_core, send_sems.at[6], recv_sems.at[6], partner)
    tail_first.start()
    tail_first.wait_recv()
    tail_half[...] = tail[rows(core, 384)] + tail_core[...]

    def tail_to_plane(i):
        qd = lax.rem(q + i + 1, 16)
        send(tail_half.at[rows(qd, 24)], tail_plane.at[i], send_sems.at[7], recv_sems.at[7], device_at(core, z8, qd)).start()

    looped(15, tail_to_plane)
    wait_for(from_z, recv_sems.at[3])

    def back_plane(i):
        send(all_z, all_plane.at[rows(q, 64)], send_sems.at[4], recv_sems.at[4], device_at(core, z8, lax.rem(q + i + 1, 16))).start()

    looped(15, back_plane)
    all_plane[rows(q, 64)] = all_z[...]
    wait_for(tail_plane, recv_sems.at[7])
    tail_part[...] = (tail_half[rows(q, 24)] + jnp.sum(tail_plane[...], axis=0)) * scale

    def tail_to_z(i):
        zd = lax.rem(z8 + i + 1, 8)
        send(tail_part, tail_z.at[z8], send_sems.at[8], recv_sems.at[8], device_at(core, zd, q)).start()

    looped(7, tail_to_z)
    tail_z[z8] = tail_part[...]
    wait_for(from_plane, recv_sems.at[4])
    last = send(all_plane, all_core, send_sems.at[5], recv_sems.at[5], partner)
    last.start()
    wait_for(tail_z.at[pl.ds(0, 7)], recv_sems.at[8])
    tail_piece[...] = jnp.sum(tail_z[...], axis=0)

    def tail_back(i):
        send(tail_piece, tail_all.at[rows(q, 24)], send_sems.at[9], recv_sems.at[9], device_at(core, z8, lax.rem(q + i + 1, 16))).start()

    looped(15, tail_back)
    tail_all[rows(q, 24)] = tail_piece[...]
    last.wait_recv()
    acc_sum[rows(core, 1024)] = all_plane[...]
    acc_sum[rows(1 - core, 1024)] = all_core[...]
    for b in range(4):
        sum_down[block(b)] = acc_sum[block(b)]
        sum_up[:, block(b)] = acc_sum[block(4 + b)]
    sum_out[...] = acc_sum[block(8)]
    sum_proj[:, gate_weight] = acc_sum[block(9)]
    sum_gain[1:3] = acc_sum[1281:1283]
    sum_bias[1:3] = acc_sum[1284:1286]
    wait_for(tail_plane, recv_sems.at[9])
    tail_last = send(tail_all, tail_other, send_sems.at[10], recv_sems.at[10], partner)
    tail_last.start()

    def put_proj(which, source):
        for k in range(2):
            terms = jnp.concatenate([source[b * 24 : b * 24 + 16] for b in range(8 * k, 8 * k + 8)], axis=0)
            sum_proj[:, column(which * 2 + k)] = terms.T

    put_proj(core, tail_all)
    tail_last.wait_recv()
    put_proj(1 - core, tail_other)
    norm_terms = jnp.where(core == 0, tail_all[16:24], tail_other[16:24])
    sum_gain[0:1] = norm_terms[0:1]
    sum_bias[0:1] = norm_terms[1:2]

    first.wait_send()
    wait_for(from_plane, send_sems.at[1])
    wait_for(from_z, send_sems.at[2])
    wait_for(from_z, send_sems.at[3])
    wait_for(from_plane, send_sems.at[4])
    last.wait_send()
    tail_first.wait_send()
    wait_for(tail_plane, send_sems.at[7])
    wait_for(tail_z.at[pl.ds(0, 7)], send_sems.at[8])
    wait_for(tail_plane, send_sems.at[9])
    tail_last.wait_send()

    def settle(j):
        wait_for(factors_in.at[j, pl.ds(0, 63)], xs.at[0, j])
        wait_for(prod_in.at[j, pl.ds(0, 63)], xs.at[1, j])
        wait_for(cots_in.at[j, pl.ds(0, 63)], xs.at[2, j])
        wait_for(grads_in.at[j, pl.ds(0, 63)], xs.at[3, j])

    looped(CHUNKS, settle)


def local(
    pair, cotangent, lengths, proj_weight, out_weight, up_weight, down_weight, norm_gain, norm_bias
):
    pair_rows = pair[0]
    cot_rows = cotangent[0]
    vmem = pl.BlockSpec(memory_space=pltpu.VMEM)
    both = (CHUNKS, 64, 2, 2, 8, 128)
    single = (CHUNKS, 64, 2, 8, 128)
    outs = pl.pallas_call(
        functools.partial(whole_kernel, 1.0 / pair_rows.shape[1]),
        out_shape=(
            jax.ShapeDtypeStruct(pair_rows.shape, BF16),
            jax.ShapeDtypeStruct(proj_weight.shape, F32),
            jax.ShapeDtypeStruct(out_weight.shape, F32),
            jax.ShapeDtypeStruct(up_weight.shape, F32),
            jax.ShapeDtypeStruct(down_weight.shape, F32),
            jax.ShapeDtypeStruct(norm_gain.shape, F32),
            jax.ShapeDtypeStruct(norm_bias.shape, F32),
        ),
        in_specs=[pl.BlockSpec(memory_space=pltpu.SMEM)] + [vmem] * 8,
        out_specs=(vmem,) * 7,
        scratch_shapes=[
            pltpu.VMEM(both, BF16),
            pltpu.VMEM(both, BF16),
            pltpu.VMEM((2, 512, 512), BF16),
            pltpu.VMEM((2, 512, 512), BF16),
            pltpu.VMEM(single, BF16),
            pltpu.VMEM(single, BF16),
            pltpu.VMEM(single, BF16),
            pltpu.VMEM(single, BF16),
            pltpu.VMEM((2, 512, 512), BF16),
            pltpu.VMEM((2, 512, 512), BF16),
            pltpu.VMEM(both, BF16),
            pltpu.VMEM(both, BF16),
            pltpu.VMEM((1024, 128), F32),
            pltpu.VMEM((1024, 128), F32),
            pltpu.VMEM((512, 128), BF16),
            pltpu.VMEM((128, 128), F32),
            pltpu.VMEM((128, 128), F32),
            pltpu.VMEM(pair_rows.shape, F32),
            pltpu.VMEM(pair_rows.shape, F32),
            pltpu.VMEM((2048, 128), F32),
            pltpu.VMEM((768, 128), F32),
            pltpu.VMEM((128, 128), F32),
            pltpu.VMEM((1024, 128), F32),
            pltpu.VMEM((15, 64, 128), F32),
            pltpu.VMEM((7, 8, 128), F32),
            pltpu.VMEM((1024, 128), F32),
            pltpu.VMEM((64, 128), F32),
            pltpu.VMEM((8, 128), F32),
            pltpu.VMEM((64, 128), F32),
            pltpu.VMEM((1024, 128), F32),
            pltpu.VMEM((1024, 128), F32),
            pltpu.VMEM((2048, 128), F32),
            pltpu.VMEM((384, 128), F32),
            pltpu.VMEM((384, 128), F32),
            pltpu.VMEM((15, 24, 128), F32),
            pltpu.VMEM((24, 128), F32),
            pltpu.VMEM((8, 24, 128), F32),
            pltpu.VMEM((24, 128), F32),
            pltpu.VMEM((384, 128), F32),
            pltpu.VMEM((384, 128), F32),
            pltpu.SemaphoreType.DMA((4, CHUNKS)),
            pltpu.SemaphoreType.DMA((4, CHUNKS)),
            pltpu.SemaphoreType.DMA((11,)),
            pltpu.SemaphoreType.DMA((11,)),
        ],
        compiler_params=pltpu.CompilerParams(
            collective_id=0, has_side_effects=True, vmem_limit_bytes=60 * 1024 * 1024
        ),
        name="whole",
    )(
        lengths,
        pair_rows,
        cot_rows,
        proj_weight,
        out_weight,
        up_weight,
        down_weight,
        norm_gain,
        norm_bias,
    )
    return (outs[0][None], *outs[1:])


def solution(mesh):
    in_specs = (
        P("crop", "row", None, None),
        P("crop", "row", None, None),
        P("crop"),
        P(),
        P(),
        P(),
        P(),
        P(),
        P(),
    )
    out_specs = (P("crop", "row", None, None), P(), P(), P(), P(), P(), P())
    return jax.shard_map(local, mesh=mesh, in_specs=in_specs, out_specs=out_specs, check_vma=False)
```

```python
import functools

import jax
import jax.numpy as jnp
from jax import lax
from jax.experimental import pallas as pl
from jax.experimental.pallas import tpu as pltpu
from jax.sharding import PartitionSpec as P

EPSILON = 1e-05
F32 = jnp.float32
BF16 = jnp.bfloat16
MESH = pl.DeviceIdType.MESH
CHUNKS = 4


def place():
    crop = lax.axis_index("crop")
    row = lax.axis_index("row")
    core = lax.rem(crop, 2)
    zhi = lax.div(crop, 2)
    q = lax.div(row, 4)
    zlo = lax.rem(row, 4)
    return core, zhi * 4 + zlo, q


def device_at(core, z, q):
    return (lax.div(z, 4) * 2 + core, q * 4 + lax.rem(z, 4))


def send(src, dst, send_sem, recv_sem, device):
    return pltpu.make_async_remote_copy(
        src_ref=src,
        dst_ref=dst,
        send_sem=send_sem,
        recv_sem=recv_sem,
        device_id=device,
        device_id_type=MESH,
    )


def wait_for(ref, sem):
    pltpu.make_async_copy(ref, ref, sem).wait()


def signal(sem, device):
    pl.semaphore_signal(sem, inc=1, device_id=device, device_id_type=MESH)


def looped(count, body):
    lax.fori_loop(0, count, lambda i, carry: (body(i), carry)[1], 0)


def peers(body):
    crop = lax.axis_index("crop")
    row = lax.axis_index("row")
    q = lax.div(row, 4)
    z = lax.rem(row, 4)

    def step(i):
        n = i + 1
        qd = lax.rem(q + lax.rem(n, 16), 16)
        zd = lax.rem(z + lax.div(n, 16), 4)
        body(qd * 4 + zd, zd * 16 + qd, lax.div(n, 16), (crop, qd * 4 + zd))

    looped(63, step)


def sigmoid(x):
    return 0.5 + 0.5 * jnp.tanh(0.5 * x)


def dot(a, b, dim_a, dim_b):
    return lax.dot_general(a, b, (((dim_a,), (dim_b,)), ((), ())), preferred_element_type=F32)


def norm(values, axis):
    center = values - jnp.mean(values, axis=axis, keepdims=True)
    inv_std = lax.rsqrt(jnp.mean(center * center, axis=axis, keepdims=True) + EPSILON)
    return center * inv_std, inv_std


def norm_back(upstream, normed, inv_std, gain, axis):
    scaled = upstream * gain
    return inv_std * (
        scaled
        - jnp.mean(scaled, axis=axis, keepdims=True)
        - normed * jnp.mean(scaled * normed, axis=axis, keepdims=True)
    )


def to_flat(turn, value):
    turn[...] = value.reshape(1024, 128)
    return jnp.concatenate([turn[pl.ds(r, 128, stride=8), :] for r in range(8)], axis=1)


def to_rows(turn, value):
    for r in range(8):
        turn[pl.ds(r, 128, stride=8), :] = value[:, r * 128 : (r + 1) * 128]
    return turn[...].reshape(128, 8, 128)


def column(j):
    return pl.ds(pl.multiple_of(j * 128, 128), 128)


def place_of(ref, j):
    return ref[:, column(j), :].reshape(1024, 128)


def rows(i, count):
    return pl.ds(pl.multiple_of(i * count, count), count)


def block(b):
    return slice(b * 128, (b + 1) * 128)


def whole_kernel(
    scale,
    lengths_ref,
    pair_ref,
    cot_ref,
    proj_ref,
    out_ref,
    up_ref,
    down_ref,
    gain_ref,
    bias_ref,
    grad_ref,
    sum_proj,
    sum_out,
    sum_up,
    sum_down,
    sum_gain,
    sum_bias,
    factors_out,
    factors_in,
    left_mat,
    right_mat,
    prod_out,
    prod_in,
    cots_out,
    cots_in,
    cot_mat,
    cot_turned,
    grads_out,
    grads_in,
    turn_a,
    turn_b,
    wt_ref,
    gain_col,
    bias_col,
    first_ref,
    gate_ref,
    acc,
    tail,
    columns,
    from_core,
    from_plane,
    from_z,
    half,
    part,
    piece,
    all_z,
    all_plane,
    all_core,
    acc_sum,
    tail_core,
    tail_half,
    tail_plane,
    tail_part,
    tail_z,
    tail_piece,
    tail_all,
    tail_other,
    entered_ref,
    factor_ref,
    plane_terms,
    natural,
    xs,
    xr,
    send_sems,
    recv_sems,
):
    core, z8, q = place()
    row = lax.axis_index("row")
    partner = device_at(1 - core, z8, q)
    barrier = pltpu.get_barrier_semaphore()
    signal(barrier, partner)
    peers(lambda dest, owner, hop, device: signal(barrier, device))
    looped(4, lambda i: signal(barrier, device_at(core, lax.rem(lax.div(z8, 4) * 4 + 4 + i, 8), q)))
    acc[...] = jnp.zeros_like(acc)
    tail[...] = jnp.zeros_like(tail)
    columns[...] = jnp.zeros_like(columns)
    for b in range(4):
        wt_ref[block(b)] = proj_ref[:, block(b)].T
    gain_col[...] = jnp.broadcast_to(gain_ref[1:2], (128, 128)).T
    bias_col[...] = jnp.broadcast_to(bias_ref[1:2], (128, 128)).T
    gain0, bias0 = gain_ref[0:1], bias_ref[0:1]
    gain2, bias2 = gain_ref[2:3], bias_ref[2:3]
    gate_weight = slice(512, 640)

    def enter(j):
        normed, inv = norm(place_of(pair_ref, j).astype(F32), 1)
        entered = (normed * gain0 + bias0).astype(BF16)
        return normed, inv, entered

    def keep_of(j):
        at = lax.broadcasted_iota(jnp.int32, (1, 1024), 1)
        row_at = row * 8 + lax.shift_right_logical(at, 7)
        col_at = j * 128 + jnp.bitwise_and(at, 127)
        return jnp.where(jnp.maximum(row_at, col_at) < lengths_ref[0], 1.0, 0.0)

    zlo = lax.rem(row, 4)
    mine = zlo * 16 + q

    def start_products(j):
        def one(dest, owner, hop, device):
            send(prod_out.at[j, dest], prod_in.at[j, mine], xs.at[1, j], xr.at[1, j], device).start()

        peers(one)
        prod_in[j, mine] = prod_out[j, row]

    def start_cots(j):
        def one(dest, owner, hop, device):
            send(cots_out.at[j, owner], cots_in.at[j, row], xs.at[2, j], xr.at[2, j], device).start()

        peers(one)
        cots_in[j, row] = cots_out[j, mine]

    def wait_chunk(n, j, dst):
        wait_for(dst.at[j, pl.ds(0, 63)], xr.at[n, j])

    def enter_chunk(j):
        _, _, entered = enter(j)
        keep = keep_of(j)
        pre = dot(wt_ref[...], entered, 1, 1)
        left = sigmoid(pre[0:128]) * pre[128:256] * keep
        right = sigmoid(pre[256:384]) * pre[384:512] * keep
        factors_out[:, 0, :, :, column(j)] = to_rows(turn_a, left).astype(BF16).reshape(64, 2, 8, 128)
        factors_out[:, 1, :, :, column(j)] = to_rows(turn_b, right).astype(BF16).reshape(64, 2, 8, 128)

    looped(CHUNKS, enter_chunk)
    pl.semaphore_wait(barrier, 68)

    def start_factors(dest, owner, hop, device):
        send(factors_out.at[owner], factors_in.at[row], xs.at[0, 0], xr.at[0, 0], device).start()

    peers(start_factors)
    factors_in[row] = factors_out[mine]
    wait_for(factors_in.at[pl.ds(0, 63)], xr.at[0, 0])

    def matrix(value):
        return value.astype(F32).reshape(512, 128)

    def gather_factors(j):
        for c in range(2):
            left_mat[c, :, column(j)] = matrix(factors_in[:, 0, c, :, column(j)]).astype(BF16)
            right_mat[c, :, column(j)] = matrix(factors_in[:, 1, c, :, column(j)]).astype(BF16)

    looped(CHUNKS, gather_factors)

    def product(j):
        for c in range(2):
            prod = dot(left_mat[c], right_mat[c, rows(j, 128), :], 1, 1)
            prod_out[j, :, c] = prod.reshape(64, 8, 128).astype(BF16)
        start_products(j)

    looped(CHUNKS, product)

    def middle(j):
        _, _, entered = enter(j)
        gate = sigmoid(dot(entered, proj_ref[:, gate_weight], 1, 0))
        cot = place_of(cot_ref, j)
        cot_t = cot.T
        wait_chunk(1, j, prod_in)
        flat = to_flat(turn_a, prod_in[j].astype(F32))
        gain1 = gain_col[:, 0:1]
        prod_normed, prod_inv = norm(flat, 0)
        prod_bf = (prod_normed * gain1 + bias_col[:, 0:1]).astype(BF16)
        update = dot(prod_bf, out_ref[...], 0, 0)
        first = (place_of(pair_ref, j).astype(F32) + gate * update).astype(BF16)
        tran_normed, tran_inv = norm(first.astype(F32), 1)
        tran_bf = (tran_normed * gain2 + bias2).astype(BF16)
        tran_t = tran_bf.T
        tran_grad = jnp.zeros((1024, 128), F32)
        for h in range(2):
            at = slice(h * 256, (h + 1) * 256)
            hidden_pre = dot(tran_bf, up_ref[:, at], 1, 0)
            hidden_sig = sigmoid(hidden_pre)
            hidden = (hidden_pre * hidden_sig).astype(BF16)
            down_term = dot(cot_t, hidden, 1, 0)
            hidden_grad = (
                dot(cot, down_ref[at, :], 1, 1)
                * hidden_sig
                * (1.0 + hidden_pre * (1.0 - hidden_sig))
            ).astype(BF16)
            up_term = dot(tran_t, hidden_grad, 1, 0)
            for k in range(2):
                acc[block(2 * h + k)] += down_term[:, block(k)]
                acc[block(4 + 2 * h + k)] += up_term[:, block(k)]
            tran_grad += dot(hidden_grad, up_ref[:, at], 1, 1)
        acc[1282:1283] += jnp.sum(tran_grad * tran_normed, axis=0, keepdims=True)
        acc[1285:1286] += jnp.sum(tran_grad, axis=0, keepdims=True)
        first_grad = norm_back(tran_grad, tran_normed, tran_inv, gain2, 1) + cot.astype(F32)
        update_grad = (first_grad * gate).astype(BF16)
        gate_grad = (first_grad * update * gate * (1.0 - gate)).astype(BF16)
        acc[block(8)] += dot(prod_bf, update_grad, 1, 0)
        norm_grad = dot(out_ref[...], update_grad, 1, 1)
        columns[:, 0:1] += jnp.sum(norm_grad * prod_normed, axis=1, keepdims=True)
        columns[:, 1:2] += jnp.sum(norm_grad, axis=1, keepdims=True)
        prod_grad = norm_back(norm_grad, prod_normed, prod_inv, gain1, 0)
        cots_out[j] = to_rows(turn_b, prod_grad).astype(BF16).reshape(64, 2, 8, 128)
        start_cots(j)
        first_ref[:, column(j), :] = first_grad.reshape(8, 128, 128)
        gate_ref[:, column(j), :] = dot(gate_grad, proj_ref[:, gate_weight], 1, 1).reshape(8, 128, 128)
        acc[block(9)] += dot(entered.T, gate_grad, 1, 0)

    looped(CHUNKS, middle)
    for b in range(4):
        acc[block(b)] = acc[block(b)].T
    turned = columns[...].T
    acc[1281:1282] = turned[0:1]
    acc[1284:1285] = turned[1:2]

    first = send(acc.at[rows(1 - core, 1024)], from_core, send_sems.at[0], recv_sems.at[0], partner)
    first.start()
    first.wait_recv()
    half[...] = acc[rows(core, 1024)] + from_core[...]

    def to_plane(i):
        qd = lax.rem(q + i + 1, 16)
        send(half.at[rows(qd, 64)], from_plane.at[i], send_sems.at[1], recv_sems.at[1], device_at(core, z8, qd)).start()

    looped(15, to_plane)

    def gather_cots(j):
        wait_chunk(2, j, cots_in)
        for c in range(2):
            grad = matrix(cots_in[j, :, c])
            cot_mat[c, :, column(j)] = grad.astype(BF16)
            cot_turned[c, rows(j, 128), :] = grad.T.astype(BF16)

    looped(CHUNKS, gather_cots)
    wait_for(from_plane, recv_sems.at[1])
    part[...] = half[rows(q, 64)] + jnp.sum(from_plane[...], axis=0)

    def to_z(i):
        zd = lax.rem(z8 + i + 1, 8)
        send(part.at[rows(zd, 8)], from_z.at[i], send_sems.at[2], recv_sems.at[2], device_at(core, zd, q)).start()

    looped(7, to_z)

    def product_grads(j):
        for c in range(2):
            left = dot(cot_mat[c], right_mat[c, :, column(j)], 1, 0)
            right = dot(cot_turned[c], left_mat[c, :, column(j)], 1, 0)
            grads_out[:, 0, c, :, column(j)] = left.reshape(64, 8, 128).astype(BF16)
            grads_out[:, 1, c, :, column(j)] = right.reshape(64, 8, 128).astype(BF16)

    looped(CHUNKS, product_grads)

    def start_grads(dest, owner, hop, device):
        send(grads_out.at[dest], grads_in.at[mine], xs.at[3, hop], xr.at[3, hop], device).start()

    peers(start_grads)
    grads_in[mine] = grads_out[row]
    wait_for(from_z, recv_sems.at[2])
    piece[...] = (part[rows(z8, 8)] + jnp.sum(from_z[...], axis=0)) * scale

    def back_z(i):
        send(piece, all_z.at[rows(z8, 8)], send_sems.at[3], recv_sems.at[3], device_at(core, lax.rem(z8 + i + 1, 8), q)).start()

    looped(7, back_z)
    all_z[rows(z8, 8)] = piece[...]

    def prepare(j):
        _, _, entered = enter(j)
        keep = keep_of(j)
        pre = dot(wt_ref[...], entered, 1, 1)
        left_sig = sigmoid(pre[0:128])
        right_sig = sigmoid(pre[256:384])
        entered_ref[j] = entered
        left_kept = left_sig * keep
        right_kept = right_sig * keep
        factor_ref[j, 0] = pre[128:256] * left_kept * (1.0 - left_sig)
        factor_ref[j, 1] = left_kept
        factor_ref[j, 2] = pre[384:512] * right_kept * (1.0 - right_sig)
        factor_ref[j, 3] = right_kept

    looped(CHUNKS, prepare)

    def plane_flat(turn, value):
        turn[0:256] = value.reshape(256, 128)
        return jnp.concatenate([turn[pl.ds(r, 32, stride=8), :] for r in range(8)], axis=1)

    def leave(hop, count):
        zs = lax.rem(zlo + 4 - hop, 4)
        wait_for(grads_in.at[pl.ds(0, count)], xr.at[3, hop])
        plane = rows(zs, 16)
        own = rows(zs, 32)
        weights = jnp.concatenate(
            [wt_ref[pl.ds(pl.multiple_of(b * 128 + zs * 32, 32), 32), :] for b in range(4)], axis=0
        )
        plane_terms[...] = jnp.zeros_like(plane_terms)

        def positions(j):
            left = plane_flat(turn_a, grads_in[plane, 0, :, :, column(j)].astype(F32))
            right = plane_flat(turn_b, grads_in[plane, 1, :, :, column(j)].astype(F32))
            factor_grad = jnp.concatenate(
                [
                    left * factor_ref[j, 0, own, :],
                    left * factor_ref[j, 1, own, :],
                    right * factor_ref[j, 2, own, :],
                    right * factor_ref[j, 3, own, :],
                ],
                axis=0,
            ).astype(BF16)
            plane_terms[...] += dot(factor_grad, entered_ref[j], 1, 0)
            gate_ref[:, column(j), :] += dot(factor_grad, weights, 0, 0).reshape(8, 128, 128)

        looped(CHUNKS, positions)
        base = lax.div(zs, 2) * 384 + lax.rem(zs, 2) * 192
        for b in range(8):
            tail[pl.ds(pl.multiple_of(base + b * 24, 8), 16)] = plane_terms[b * 16 : b * 16 + 16]

    leave(0, 15)
    looped(3, lambda i: leave(i + 1, 16))

    def finish(j):
        normed, inv, _ = enter(j)
        input_grad = place_of(gate_ref, j)
        tail[16:17] += jnp.sum(input_grad * normed, axis=0, keepdims=True)
        tail[17:18] += jnp.sum(input_grad, axis=0, keepdims=True)
        result = norm_back(input_grad, normed, inv, gain0, 1) + place_of(first_ref, j)
        grad_ref[:, column(j), :] = result.astype(BF16).reshape(8, 128, 128)

    looped(CHUNKS, finish)

    tail_first = send(tail.at[rows(1 - core, 384)], tail_core, send_sems.at[6], recv_sems.at[6], partner)
    tail_first.start()
    tail_first.wait_recv()
    tail_half[...] = tail[rows(core, 384)] + tail_core[...]

    def tail_to_plane(i):
        qd = lax.rem(q + i + 1, 16)
        send(tail_half.at[rows(qd, 24)], tail_plane.at[i], send_sems.at[7], recv_sems.at[7], device_at(core, z8, qd)).start()

    looped(15, tail_to_plane)
    wait_for(from_z, recv_sems.at[3])

    def back_plane(i):
        send(all_z, all_plane.at[rows(q, 64)], send_sems.at[4], recv_sems.at[4], device_at(core, z8, lax.rem(q + i + 1, 16))).start()

    looped(15, back_plane)
    all_plane[rows(q, 64)] = all_z[...]
    wait_for(tail_plane, recv_sems.at[7])
    tail_part[...] = (tail_half[rows(q, 24)] + jnp.sum(tail_plane[...], axis=0)) * scale

    def tail_to_z(i):
        zd = lax.rem(z8 + i + 1, 8)
        send(tail_part, tail_z.at[z8], send_sems.at[8], recv_sems.at[8], device_at(core, zd, q)).start()

    looped(7, tail_to_z)
    tail_z[z8] = tail_part[...]
    wait_for(from_plane, recv_sems.at[4])
    last = send(all_plane, all_core, send_sems.at[5], recv_sems.at[5], partner)
    last.start()
    wait_for(tail_z.at[pl.ds(0, 7)], recv_sems.at[8])
    tail_piece[...] = jnp.sum(tail_z[...], axis=0)

    def tail_back(i):
        send(tail_piece, tail_all.at[rows(q, 24)], send_sems.at[9], recv_sems.at[9], device_at(core, z8, lax.rem(q + i + 1, 16))).start()

    looped(15, tail_back)
    tail_all[rows(q, 24)] = tail_piece[...]
    last.wait_recv()
    acc_sum[rows(core, 1024)] = all_plane[...]
    acc_sum[rows(1 - core, 1024)] = all_core[...]
    for b in range(4):
        sum_down[block(b)] = acc_sum[block(b)]
        sum_up[:, block(b)] = acc_sum[block(4 + b)]
    sum_out[...] = acc_sum[block(8)]
    sum_proj[:, gate_weight] = acc_sum[block(9)]
    sum_gain[1:3] = acc_sum[1281:1283]
    sum_bias[1:3] = acc_sum[1284:1286]
    wait_for(tail_plane, recv_sems.at[9])
    tail_last = send(tail_all, tail_other, send_sems.at[10], recv_sems.at[10], partner)
    tail_last.start()

    def put_proj(which, source):
        for k in range(8):
            at = pl.multiple_of((k % 4) * 128 + (which * 2 + k // 4) * 32, 32)
            natural[pl.ds(at, 16)] = source[48 * k : 48 * k + 16]
            natural[pl.ds(at + 16, 16)] = source[48 * k + 24 : 48 * k + 40]

    put_proj(core, tail_all)
    tail_last.wait_recv()
    put_proj(1 - core, tail_other)
    for b in range(4):
        sum_proj[:, block(b)] = natural[block(b)].T
    norm_terms = jnp.where(core == 0, tail_all[16:24], tail_other[16:24])
    sum_gain[0:1] = norm_terms[0:1]
    sum_bias[0:1] = norm_terms[1:2]

    first.wait_send()
    wait_for(from_plane, send_sems.at[1])
    wait_for(from_z, send_sems.at[2])
    wait_for(from_z, send_sems.at[3])
    wait_for(from_plane, send_sems.at[4])
    last.wait_send()
    tail_first.wait_send()
    wait_for(tail_plane, send_sems.at[7])
    wait_for(tail_z.at[pl.ds(0, 7)], send_sems.at[8])
    wait_for(tail_plane, send_sems.at[9])
    tail_last.wait_send()

    def settle(j):
        wait_for(prod_in.at[j, pl.ds(0, 63)], xs.at[1, j])
        wait_for(cots_in.at[j, pl.ds(0, 63)], xs.at[2, j])

    looped(CHUNKS, settle)
    wait_for(factors_in.at[pl.ds(0, 63)], xs.at[0, 0])
    wait_for(grads_in.at[pl.ds(0, 15)], xs.at[3, 0])
    looped(3, lambda i: wait_for(grads_in.at[pl.ds(0, 16)], xs.at[3, i + 1]))


def local(
    pair, cotangent, lengths, proj_weight, out_weight, up_weight, down_weight, norm_gain, norm_bias
):
    pair_rows = pair[0]
    cot_rows = cotangent[0]
    vmem = pl.BlockSpec(memory_space=pltpu.VMEM)
    both = (64, 2, 2, 8, 512)
    single = (CHUNKS, 64, 2, 8, 128)
    outs = pl.pallas_call(
        functools.partial(whole_kernel, 1.0 / pair_rows.shape[1]),
        out_shape=(
            jax.ShapeDtypeStruct(pair_rows.shape, BF16),
            jax.ShapeDtypeStruct(proj_weight.shape, F32),
            jax.ShapeDtypeStruct(out_weight.shape, F32),
            jax.ShapeDtypeStruct(up_weight.shape, F32),
            jax.ShapeDtypeStruct(down_weight.shape, F32),
            jax.ShapeDtypeStruct(norm_gain.shape, F32),
            jax.ShapeDtypeStruct(norm_bias.shape, F32),
        ),
        in_specs=[pl.BlockSpec(memory_space=pltpu.SMEM)] + [vmem] * 8,
        out_specs=(vmem,) * 7,
        scratch_shapes=[
            pltpu.VMEM(both, BF16),
            pltpu.VMEM(both, BF16),
            pltpu.VMEM((2, 512, 512), BF16),
            pltpu.VMEM((2, 512, 512), BF16),
            pltpu.VMEM(single, BF16),
            pltpu.VMEM(single, BF16),
            pltpu.VMEM(single, BF16),
            pltpu.VMEM(single, BF16),
            pltpu.VMEM((2, 512, 512), BF16),
            pltpu.VMEM((2, 512, 512), BF16),
            pltpu.VMEM(both, BF16),
            pltpu.VMEM(both, BF16),
            pltpu.VMEM((1024, 128), F32),
            pltpu.VMEM((1024, 128), F32),
            pltpu.VMEM((512, 128), BF16),
            pltpu.VMEM((128, 128), F32),
            pltpu.VMEM((128, 128), F32),
            pltpu.VMEM(pair_rows.shape, F32),
            pltpu.VMEM(pair_rows.shape, F32),
            pltpu.VMEM((2048, 128), F32),
            pltpu.VMEM((768, 128), F32),
            pltpu.VMEM((128, 128), F32),
            pltpu.VMEM((1024, 128), F32),
            pltpu.VMEM((15, 64, 128), F32),
            pltpu.VMEM((7, 8, 128), F32),
            pltpu.VMEM((1024, 128), F32),
            pltpu.VMEM((64, 128), F32),
            pltpu.VMEM((8, 128), F32),
            pltpu.VMEM((64, 128), F32),
            pltpu.VMEM((1024, 128), F32),
            pltpu.VMEM((1024, 128), F32),
            pltpu.VMEM((2048, 128), F32),
            pltpu.VMEM((384, 128), F32),
            pltpu.VMEM((384, 128), F32),
            pltpu.VMEM((15, 24, 128), F32),
            pltpu.VMEM((24, 128), F32),
            pltpu.VMEM((8, 24, 128), F32),
            pltpu.VMEM((24, 128), F32),
            pltpu.VMEM((384, 128), F32),
            pltpu.VMEM((384, 128), F32),
            pltpu.VMEM((CHUNKS, 1024, 128), BF16),
            pltpu.VMEM((CHUNKS, 4, 128, 1024), F32),
            pltpu.VMEM((128, 128), F32),
            pltpu.VMEM((512, 128), F32),
            pltpu.SemaphoreType.DMA((4, CHUNKS)),
            pltpu.SemaphoreType.DMA((4, CHUNKS)),
            pltpu.SemaphoreType.DMA((11,)),
            pltpu.SemaphoreType.DMA((11,)),
        ],
        compiler_params=pltpu.CompilerParams(
            collective_id=0, has_side_effects=True, vmem_limit_bytes=60 * 1024 * 1024
        ),
        name="whole",
    )(
        lengths,
        pair_rows,
        cot_rows,
        proj_weight,
        out_weight,
        up_weight,
        down_weight,
        norm_gain,
        norm_bias,
    )
    return (outs[0][None], *outs[1:])


def solution(mesh):
    in_specs = (
        P("crop", "row", None, None),
        P("crop", "row", None, None),
        P("crop"),
        P(),
        P(),
        P(),
        P(),
        P(),
        P(),
    )
    out_specs = (P("crop", "row", None, None), P(), P(), P(), P(), P(), P())
    return jax.shard_map(local, mesh=mesh, in_specs=in_specs, out_specs=out_specs, check_vma=False)
```

```python
import functools

import jax
import jax.numpy as jnp
from jax import lax
from jax.experimental import pallas as pl
from jax.experimental.pallas import tpu as pltpu
from jax.sharding import PartitionSpec as P

EPSILON = 1e-05
F32 = jnp.float32
BF16 = jnp.bfloat16
MESH = pl.DeviceIdType.MESH
CHUNKS = 4


def place():
    crop = lax.axis_index("crop")
    row = lax.axis_index("row")
    core = lax.rem(crop, 2)
    zhi = lax.div(crop, 2)
    q = lax.div(row, 4)
    zlo = lax.rem(row, 4)
    return core, zhi * 4 + zlo, q


def device_at(core, z, q):
    return (lax.div(z, 4) * 2 + core, q * 4 + lax.rem(z, 4))


def send(src, dst, send_sem, recv_sem, device):
    return pltpu.make_async_remote_copy(
        src_ref=src,
        dst_ref=dst,
        send_sem=send_sem,
        recv_sem=recv_sem,
        device_id=device,
        device_id_type=MESH,
    )


def wait_for(ref, sem):
    pltpu.make_async_copy(ref, ref, sem).wait()


def signal(sem, device):
    pl.semaphore_signal(sem, inc=1, device_id=device, device_id_type=MESH)


def looped(count, body):
    lax.fori_loop(0, count, lambda i, carry: (body(i), carry)[1], 0)


def peers(body):
    crop = lax.axis_index("crop")
    row = lax.axis_index("row")
    q = lax.div(row, 4)
    z = lax.rem(row, 4)

    def step(i):
        n = i + 1
        dest = lax.rem(q + lax.rem(n, 16), 16) * 4 + lax.rem(z + lax.div(n, 16), 4)
        body(dest, (crop, dest))

    looped(63, step)


def sigmoid(x):
    return 0.5 + 0.5 * jnp.tanh(0.5 * x)


def dot(a, b, dim_a, dim_b):
    return lax.dot_general(a, b, (((dim_a,), (dim_b,)), ((), ())), preferred_element_type=F32)


def norm(values, axis):
    center = values - jnp.mean(values, axis=axis, keepdims=True)
    inv_std = lax.rsqrt(jnp.mean(center * center, axis=axis, keepdims=True) + EPSILON)
    return center * inv_std, inv_std


def norm_back(upstream, normed, inv_std, gain, axis):
    scaled = upstream * gain
    return inv_std * (
        scaled
        - jnp.mean(scaled, axis=axis, keepdims=True)
        - normed * jnp.mean(scaled * normed, axis=axis, keepdims=True)
    )


def to_flat(turn, value):
    turn[...] = value.reshape(1024, 128)
    return jnp.concatenate([turn[pl.ds(r, 128, stride=8), :] for r in range(8)], axis=1)


def to_rows(turn, value):
    for r in range(8):
        turn[pl.ds(r, 128, stride=8), :] = value[:, r * 128 : (r + 1) * 128]
    return turn[...].reshape(128, 8, 128)


def column(j):
    return pl.ds(pl.multiple_of(j * 128, 128), 128)


def place_of(ref, j):
    return ref[:, column(j), :].reshape(1024, 128)


def rows(i, count):
    return pl.ds(pl.multiple_of(i * count, count), count)


def block(b):
    return slice(b * 128, (b + 1) * 128)


def whole_kernel(
    scale,
    lengths_ref,
    pair_ref,
    cot_ref,
    proj_ref,
    out_ref,
    up_ref,
    down_ref,
    gain_ref,
    bias_ref,
    grad_ref,
    sum_proj,
    sum_out,
    sum_up,
    sum_down,
    sum_gain,
    sum_bias,
    factors_out,
    factors_in,
    left_mat,
    right_mat,
    prod_out,
    prod_in,
    cots_out,
    cots_in,
    cot_mat,
    cot_turned,
    grads_out,
    grads_in,
    turn_a,
    turn_b,
    wt_ref,
    gain_col,
    bias_col,
    first_ref,
    gate_ref,
    acc,
    tail,
    columns,
    from_core,
    from_plane,
    from_z,
    half,
    part,
    piece,
    all_z,
    all_plane,
    all_core,
    acc_sum,
    tail_core,
    tail_half,
    tail_plane,
    tail_part,
    tail_z,
    tail_piece,
    tail_all,
    tail_other,
    xs,
    xr,
    send_sems,
    recv_sems,
):
    core, z8, q = place()
    row = lax.axis_index("row")
    partner = device_at(1 - core, z8, q)
    barrier = pltpu.get_barrier_semaphore()
    signal(barrier, partner)
    peers(lambda dest, device: signal(barrier, device))
    looped(4, lambda i: signal(barrier, device_at(core, lax.rem(lax.div(z8, 4) * 4 + 4 + i, 8), q)))
    acc[...] = jnp.zeros_like(acc)
    tail[...] = jnp.zeros_like(tail)
    columns[...] = jnp.zeros_like(columns)
    for b in range(4):
        wt_ref[block(b)] = proj_ref[:, block(b)].T
    gain_col[...] = jnp.broadcast_to(gain_ref[1:2], (128, 128)).T
    bias_col[...] = jnp.broadcast_to(bias_ref[1:2], (128, 128)).T
    gain0, bias0 = gain_ref[0:1], bias_ref[0:1]
    gain2, bias2 = gain_ref[2:3], bias_ref[2:3]
    gate_weight = slice(512, 640)

    def enter(j):
        normed, inv = norm(place_of(pair_ref, j).astype(F32), 1)
        entered = (normed * gain0 + bias0).astype(BF16)
        return normed, inv, entered

    def keep_of(j):
        at = lax.broadcasted_iota(jnp.int32, (1, 1024), 1)
        row_at = row * 8 + lax.shift_right_logical(at, 7)
        col_at = j * 128 + jnp.bitwise_and(at, 127)
        return jnp.where(jnp.maximum(row_at, col_at) < lengths_ref[0], 1.0, 0.0)

    def start_chunk(n, j, src, dst):
        def one(dest, device):
            send(src.at[j, dest], dst.at[j, row], xs.at[n, j], xr.at[n, j], device).start()

        peers(one)
        dst[j, row] = src[j, row]

    def wait_chunk(n, j, dst):
        wait_for(dst.at[j, pl.ds(0, 63)], xr.at[n, j])

    def enter_chunk(j):
        _, _, entered = enter(j)
        keep = keep_of(j)
        pre = dot(wt_ref[...], entered, 1, 1)
        left = sigmoid(pre[0:128]) * pre[128:256] * keep
        right = sigmoid(pre[256:384]) * pre[384:512] * keep
        factors_out[j, :, 0] = to_rows(turn_a, left).astype(BF16).reshape(64, 2, 8, 128)
        factors_out[j, :, 1] = to_rows(turn_b, right).astype(BF16).reshape(64, 2, 8, 128)

        @pl.when(j == 0)
        def _():
            pl.semaphore_wait(barrier, 68)

        start_chunk(0, j, factors_out, factors_in)

    looped(CHUNKS, enter_chunk)

    def matrix(value):
        return value.astype(F32).reshape(512, 128)

    def gather_factors(j):
        wait_chunk(0, j, factors_in)
        for c in range(2):
            left_mat[c, :, column(j)] = matrix(factors_in[j, :, 0, c]).astype(BF16)
            right_mat[c, :, column(j)] = matrix(factors_in[j, :, 1, c]).astype(BF16)

    looped(CHUNKS, gather_factors)

    def product(j):
        for c in range(2):
            prod = dot(left_mat[c], right_mat[c, rows(j, 128), :], 1, 1)
            prod_out[j, :, c] = prod.reshape(64, 8, 128).astype(BF16)
        start_chunk(1, j, prod_out, prod_in)

    looped(CHUNKS, product)

    def middle(j):
        _, _, entered = enter(j)
        gate = sigmoid(dot(entered, proj_ref[:, gate_weight], 1, 0))
        cot = place_of(cot_ref, j)
        cot_t = cot.T
        wait_chunk(1, j, prod_in)
        flat = to_flat(turn_a, prod_in[j].astype(F32))
        gain1 = gain_col[:, 0:1]
        prod_normed, prod_inv = norm(flat, 0)
        prod_bf = (prod_normed * gain1 + bias_col[:, 0:1]).astype(BF16)
        update = dot(prod_bf, out_ref[...], 0, 0)
        first = (place_of(pair_ref, j).astype(F32) + gate * update).astype(BF16)
        tran_normed, tran_inv = norm(first.astype(F32), 1)
        tran_bf = (tran_normed * gain2 + bias2).astype(BF16)
        tran_t = tran_bf.T
        tran_grad = jnp.zeros((1024, 128), F32)
        for h in range(2):
            at = slice(h * 256, (h + 1) * 256)
            hidden_pre = dot(tran_bf, up_ref[:, at], 1, 0)
            hidden_sig = sigmoid(hidden_pre)
            hidden = (hidden_pre * hidden_sig).astype(BF16)
            down_term = dot(cot_t, hidden, 1, 0)
            hidden_grad = (
                dot(cot, down_ref[at, :], 1, 1)
                * hidden_sig
                * (1.0 + hidden_pre * (1.0 - hidden_sig))
            ).astype(BF16)
            up_term = dot(tran_t, hidden_grad, 1, 0)
            for k in range(2):
                acc[block(2 * h + k)] += down_term[:, block(k)]
                acc[block(4 + 2 * h + k)] += up_term[:, block(k)]
            tran_grad += dot(hidden_grad, up_ref[:, at], 1, 1)
        acc[1282:1283] += jnp.sum(tran_grad * tran_normed, axis=0, keepdims=True)
        acc[1285:1286] += jnp.sum(tran_grad, axis=0, keepdims=True)
        first_grad = norm_back(tran_grad, tran_normed, tran_inv, gain2, 1) + cot.astype(F32)
        update_grad = (first_grad * gate).astype(BF16)
        gate_grad = (first_grad * update * gate * (1.0 - gate)).astype(BF16)
        acc[block(8)] += dot(prod_bf, update_grad, 1, 0)
        norm_grad = dot(out_ref[...], update_grad, 1, 1)
        columns[:, 0:1] += jnp.sum(norm_grad * prod_normed, axis=1, keepdims=True)
        columns[:, 1:2] += jnp.sum(norm_grad, axis=1, keepdims=True)
        prod_grad = norm_back(norm_grad, prod_normed, prod_inv, gain1, 0)
        cots_out[j] = to_rows(turn_b, prod_grad).astype(BF16).reshape(64, 2, 8, 128)
        start_chunk(2, j, cots_out, cots_in)
        first_ref[:, column(j), :] = first_grad.reshape(8, 128, 128)
        gate_ref[:, column(j), :] = dot(gate_grad, proj_ref[:, gate_weight], 1, 1).reshape(8, 128, 128)
        acc[block(9)] += dot(entered.T, gate_grad, 1, 0)

    looped(CHUNKS, middle)
    for b in range(4):
        acc[block(b)] = acc[block(b)].T
    turned = columns[...].T
    acc[1281:1282] = turned[0:1]
    acc[1284:1285] = turned[1:2]

    first = send(acc.at[rows(1 - core, 1024)], from_core, send_sems.at[0], recv_sems.at[0], partner)
    first.start()
    first.wait_recv()
    half[...] = acc[rows(core, 1024)] + from_core[...]

    def to_plane(i):
        qd = lax.rem(q + i + 1, 16)
        send(half.at[rows(qd, 64)], from_plane.at[i], send_sems.at[1], recv_sems.at[1], device_at(core, z8, qd)).start()

    looped(15, to_plane)

    def gather_cots(j):
        wait_chunk(2, j, cots_in)
        for c in range(2):
            grad = matrix(cots_in[j, :, c])
            cot_mat[c, :, column(j)] = grad.astype(BF16)
            cot_turned[c, rows(j, 128), :] = grad.T.astype(BF16)

    looped(CHUNKS, gather_cots)
    wait_for(from_plane, recv_sems.at[1])
    part[...] = half[rows(q, 64)] + jnp.sum(from_plane[...], axis=0)

    def to_z(i):
        zd = lax.rem(z8 + i + 1, 8)
        send(part.at[rows(zd, 8)], from_z.at[i], send_sems.at[2], recv_sems.at[2], device_at(core, zd, q)).start()

    looped(7, to_z)

    def product_grads(j):
        for c in range(2):
            left = dot(cot_mat[c], right_mat[c, :, column(j)], 1, 0)
            right = dot(cot_turned[c], left_mat[c, :, column(j)], 1, 0)
            grads_out[j, :, 0, c] = left.reshape(64, 8, 128).astype(BF16)
            grads_out[j, :, 1, c] = right.reshape(64, 8, 128).astype(BF16)
        start_chunk(3, j, grads_out, grads_in)

    looped(CHUNKS, product_grads)
    wait_for(from_z, recv_sems.at[2])
    piece[...] = (part[rows(z8, 8)] + jnp.sum(from_z[...], axis=0)) * scale

    def back_z(i):
        send(piece, all_z.at[rows(z8, 8)], send_sems.at[3], recv_sems.at[3], device_at(core, lax.rem(z8 + i + 1, 8), q)).start()

    looped(7, back_z)
    all_z[rows(z8, 8)] = piece[...]

    def leave(j):
        normed, inv, entered = enter(j)
        keep = keep_of(j)
        pre = dot(wt_ref[...], entered, 1, 1)
        left_sig = sigmoid(pre[0:128])
        right_sig = sigmoid(pre[256:384])
        wait_chunk(3, j, grads_in)
        left = to_flat(turn_a, grads_in[j, :, 0].astype(F32)) * keep
        right = to_flat(turn_b, grads_in[j, :, 1].astype(F32)) * keep
        factor_grad = jnp.concatenate(
            [
                (left * pre[128:256] * left_sig * (1.0 - left_sig)).astype(BF16),
                (left * left_sig).astype(BF16),
                (right * pre[384:512] * right_sig * (1.0 - right_sig)).astype(BF16),
                (right * right_sig).astype(BF16),
            ],
            axis=0,
        )
        terms = dot(factor_grad, entered, 1, 0)
        for core_half in range(2):
            for b in range(16):
                at = core_half * 256 + b * 16
                to = core_half * 384 + b * 24
                tail[to : to + 16] += terms[at : at + 16]
        input_grad = dot(factor_grad, wt_ref[...], 0, 0) + place_of(gate_ref, j)
        tail[16:17] += jnp.sum(input_grad * normed, axis=0, keepdims=True)
        tail[17:18] += jnp.sum(input_grad, axis=0, keepdims=True)
        result = norm_back(input_grad, normed, inv, gain0, 1) + place_of(first_ref, j)
        grad_ref[:, column(j), :] = result.astype(BF16).reshape(8, 128, 128)

    looped(CHUNKS, leave)

    tail_first = send(tail.at[rows(1 - core, 384)], tail_core, send_sems.at[6], recv_sems.at[6], partner)
    tail_first.start()
    tail_first.wait_recv()
    tail_half[...] = tail[rows(core, 384)] + tail_core[...]

    def tail_to_plane(i):
        qd = lax.rem(q + i + 1, 16)
        send(tail_half.at[rows(qd, 24)], tail_plane.at[i], send_sems.at[7], recv_sems.at[7], device_at(core, z8, qd)).start()

    looped(15, tail_to_plane)
    wait_for(from_z, recv_sems.at[3])

    def back_plane(i):
        send(all_z, all_plane.at[rows(q, 64)], send_sems.at[4], recv_sems.at[4], device_at(core, z8, lax.rem(q + i + 1, 16))).start()

    looped(15, back_plane)
    all_plane[rows(q, 64)] = all_z[...]
    wait_for(tail_plane, recv_sems.at[7])
    tail_part[...] = (tail_half[rows(q, 24)] + jnp.sum(tail_plane[...], axis=0)) * scale

    def tail_to_z(i):
        zd = lax.rem(z8 + i + 1, 8)
        send(tail_part, tail_z.at[z8], send_sems.at[8], recv_sems.at[8], device_at(core, zd, q)).start()

    looped(7, tail_to_z)
    tail_z[z8] = tail_part[...]
    wait_for(from_plane, recv_sems.at[4])
    last = send(all_plane, all_core, send_sems.at[5], recv_sems.at[5], partner)
    last.start()
    wait_for(tail_z.at[pl.ds(0, 7)], recv_sems.at[8])
    tail_piece[...] = jnp.sum(tail_z[...], axis=0)

    def tail_back(i):
        send(tail_piece, tail_all.at[rows(q, 24)], send_sems.at[9], recv_sems.at[9], device_at(core, z8, lax.rem(q + i + 1, 16))).start()

    looped(15, tail_back)
    tail_all[rows(q, 24)] = tail_piece[...]
    last.wait_recv()
    acc_sum[rows(core, 1024)] = all_plane[...]
    acc_sum[rows(1 - core, 1024)] = all_core[...]
    for b in range(4):
        sum_down[block(b)] = acc_sum[block(b)]
        sum_up[:, block(b)] = acc_sum[block(4 + b)]
    sum_out[...] = acc_sum[block(8)]
    sum_proj[:, gate_weight] = acc_sum[block(9)]
    sum_gain[1:3] = acc_sum[1281:1283]
    sum_bias[1:3] = acc_sum[1284:1286]
    wait_for(tail_plane, recv_sems.at[9])
    tail_last = send(tail_all, tail_other, send_sems.at[10], recv_sems.at[10], partner)
    tail_last.start()

    def put_proj(which, source):
        for k in range(2):
            terms = jnp.concatenate([source[b * 24 : b * 24 + 16] for b in range(8 * k, 8 * k + 8)], axis=0)
            sum_proj[:, column(which * 2 + k)] = terms.T

    put_proj(core, tail_all)
    tail_last.wait_recv()
    put_proj(1 - core, tail_other)
    norm_terms = jnp.where(core == 0, tail_all[16:24], tail_other[16:24])
    sum_gain[0:1] = norm_terms[0:1]
    sum_bias[0:1] = norm_terms[1:2]

    first.wait_send()
    wait_for(from_plane, send_sems.at[1])
    wait_for(from_z, send_sems.at[2])
    wait_for(from_z, send_sems.at[3])
    wait_for(from_plane, send_sems.at[4])
    last.wait_send()
    tail_first.wait_send()
    wait_for(tail_plane, send_sems.at[7])
    wait_for(tail_z.at[pl.ds(0, 7)], send_sems.at[8])
    wait_for(tail_plane, send_sems.at[9])
    tail_last.wait_send()

    def settle(j):
        wait_for(factors_in.at[j, pl.ds(0, 63)], xs.at[0, j])
        wait_for(prod_in.at[j, pl.ds(0, 63)], xs.at[1, j])
        wait_for(cots_in.at[j, pl.ds(0, 63)], xs.at[2, j])
        wait_for(grads_in.at[j, pl.ds(0, 63)], xs.at[3, j])

    looped(CHUNKS, settle)


def hand_over(*refs):
    count = len(refs) // 2
    for source, target in zip(refs[:count], refs[count:]):
        target[...] = source[...]


def local(
    pair, cotangent, lengths, proj_weight, out_weight, up_weight, down_weight, norm_gain, norm_bias
):
    pair_rows = pair[0]
    cot_rows = cotangent[0]
    vmem = pl.BlockSpec(memory_space=pltpu.VMEM)
    both = (CHUNKS, 64, 2, 2, 8, 128)
    single = (CHUNKS, 64, 2, 8, 128)
    outs = pl.pallas_call(
        functools.partial(whole_kernel, 1.0 / pair_rows.shape[1]),
        out_shape=(
            jax.ShapeDtypeStruct(pair_rows.shape, BF16),
            jax.ShapeDtypeStruct(proj_weight.shape, F32),
            jax.ShapeDtypeStruct(out_weight.shape, F32),
            jax.ShapeDtypeStruct(up_weight.shape, F32),
            jax.ShapeDtypeStruct(down_weight.shape, F32),
            jax.ShapeDtypeStruct(norm_gain.shape, F32),
            jax.ShapeDtypeStruct(norm_bias.shape, F32),
        ),
        in_specs=[pl.BlockSpec(memory_space=pltpu.SMEM)] + [vmem] * 8,
        out_specs=(vmem,) * 7,
        scratch_shapes=[
            pltpu.VMEM(both, BF16),
            pltpu.VMEM(both, BF16),
            pltpu.VMEM((2, 512, 512), BF16),
            pltpu.VMEM((2, 512, 512), BF16),
            pltpu.VMEM(single, BF16),
            pltpu.VMEM(single, BF16),
            pltpu.VMEM(single, BF16),
            pltpu.VMEM(single, BF16),
            pltpu.VMEM((2, 512, 512), BF16),
            pltpu.VMEM((2, 512, 512), BF16),
            pltpu.VMEM(both, BF16),
            pltpu.VMEM(both, BF16),
            pltpu.VMEM((1024, 128), F32),
            pltpu.VMEM((1024, 128), F32),
            pltpu.VMEM((512, 128), BF16),
            pltpu.VMEM((128, 128), F32),
            pltpu.VMEM((128, 128), F32),
            pltpu.VMEM(pair_rows.shape, F32),
            pltpu.VMEM(pair_rows.shape, F32),
            pltpu.VMEM((2048, 128), F32),
            pltpu.VMEM((768, 128), F32),
            pltpu.VMEM((128, 128), F32),
            pltpu.VMEM((1024, 128), F32),
            pltpu.VMEM((15, 64, 128), F32),
            pltpu.VMEM((7, 8, 128), F32),
            pltpu.VMEM((1024, 128), F32),
            pltpu.VMEM((64, 128), F32),
            pltpu.VMEM((8, 128), F32),
            pltpu.VMEM((64, 128), F32),
            pltpu.VMEM((1024, 128), F32),
            pltpu.VMEM((1024, 128), F32),
            pltpu.VMEM((2048, 128), F32),
            pltpu.VMEM((384, 128), F32),
            pltpu.VMEM((384, 128), F32),
            pltpu.VMEM((15, 24, 128), F32),
            pltpu.VMEM((24, 128), F32),
            pltpu.VMEM((8, 24, 128), F32),
            pltpu.VMEM((24, 128), F32),
            pltpu.VMEM((384, 128), F32),
            pltpu.VMEM((384, 128), F32),
            pltpu.SemaphoreType.DMA((4, CHUNKS)),
            pltpu.SemaphoreType.DMA((4, CHUNKS)),
            pltpu.SemaphoreType.DMA((11,)),
            pltpu.SemaphoreType.DMA((11,)),
        ],
        compiler_params=pltpu.CompilerParams(
            collective_id=0, has_side_effects=True, vmem_limit_bytes=60 * 1024 * 1024
        ),
        name="whole",
    )(
        lengths,
        pair_rows,
        cot_rows,
        proj_weight,
        out_weight,
        up_weight,
        down_weight,
        norm_gain,
        norm_bias,
    )
    outs = pl.pallas_call(
        hand_over,
        out_shape=tuple(jax.ShapeDtypeStruct(o.shape, o.dtype) for o in outs),
        in_specs=[vmem] * 7,
        out_specs=(vmem,) * 7,
        name="hand_over",
    )(*outs)
    return (outs[0][None], *outs[1:])


def solution(mesh):
    in_specs = (
        P("crop", "row", None, None),
        P("crop", "row", None, None),
        P("crop"),
        P(),
        P(),
        P(),
        P(),
        P(),
        P(),
    )
    out_specs = (P("crop", "row", None, None), P(), P(), P(), P(), P(), P())
    return jax.shard_map(local, mesh=mesh, in_specs=in_specs, out_specs=out_specs, check_vma=False)
```

```python
import functools

import jax
import jax.numpy as jnp
from jax import lax
from jax.experimental import pallas as pl
from jax.experimental.pallas import tpu as pltpu
from jax.sharding import PartitionSpec as P

EPSILON = 1e-05
F32 = jnp.float32
BF16 = jnp.bfloat16
MESH = pl.DeviceIdType.MESH
CHUNKS = 4


def place():
    crop = lax.axis_index("crop")
    row = lax.axis_index("row")
    core = lax.rem(crop, 2)
    zhi = lax.div(crop, 2)
    q = lax.div(row, 4)
    zlo = lax.rem(row, 4)
    return core, zhi * 4 + zlo, q


def device_at(core, z, q):
    return (lax.div(z, 4) * 2 + core, q * 4 + lax.rem(z, 4))


def send(src, dst, send_sem, recv_sem, device):
    return pltpu.make_async_remote_copy(
        src_ref=src,
        dst_ref=dst,
        send_sem=send_sem,
        recv_sem=recv_sem,
        device_id=device,
        device_id_type=MESH,
    )


def wait_for(ref, sem):
    pltpu.make_async_copy(ref, ref, sem).wait()


def signal(sem, device):
    pl.semaphore_signal(sem, inc=1, device_id=device, device_id_type=MESH)


def looped(count, body):
    lax.fori_loop(0, count, lambda i, carry: (body(i), carry)[1], 0)


def peers(body):
    crop = lax.axis_index("crop")
    row = lax.axis_index("row")
    q = lax.div(row, 4)
    z = lax.rem(row, 4)

    def step(i):
        n = i + 1
        dest = lax.rem(q + lax.rem(n, 16), 16) * 4 + lax.rem(z + lax.div(n, 16), 4)
        body(dest, (crop, dest))

    def steps(i):
        for k in range(7):
            step(i * 7 + k)

    looped(9, steps)


def sigmoid(x):
    return 0.5 + 0.5 * jnp.tanh(0.5 * x)


def dot(a, b, dim_a, dim_b):
    return lax.dot_general(a, b, (((dim_a,), (dim_b,)), ((), ())), preferred_element_type=F32)


def norm(values, axis):
    center = values - jnp.mean(values, axis=axis, keepdims=True)
    inv_std = lax.rsqrt(jnp.mean(center * center, axis=axis, keepdims=True) + EPSILON)
    return center * inv_std, inv_std


def norm_back(upstream, normed, inv_std, gain, axis):
    scaled = upstream * gain
    return inv_std * (
        scaled
        - jnp.mean(scaled, axis=axis, keepdims=True)
        - normed * jnp.mean(scaled * normed, axis=axis, keepdims=True)
    )


def to_flat(turn, value):
    turn[...] = value.reshape(1024, 128)
    return jnp.concatenate([turn[pl.ds(r, 128, stride=8), :] for r in range(8)], axis=1)


def to_rows(turn, value):
    for r in range(8):
        turn[pl.ds(r, 128, stride=8), :] = value[:, r * 128 : (r + 1) * 128]
    return turn[...].reshape(128, 8, 128)


def column(j):
    return pl.ds(pl.multiple_of(j * 128, 128), 128)


def place_of(ref, j):
    return ref[:, column(j), :].reshape(1024, 128)


def rows(i, count):
    return pl.ds(pl.multiple_of(i * count, count), count)


def block(b):
    return slice(b * 128, (b + 1) * 128)


def whole_kernel(
    scale,
    lengths_ref,
    pair_ref,
    cot_ref,
    proj_ref,
    out_ref,
    up_ref,
    down_ref,
    gain_ref,
    bias_ref,
    grad_ref,
    sum_proj,
    sum_out,
    sum_up,
    sum_down,
    sum_gain,
    sum_bias,
    factors_out,
    factors_in,
    left_mat,
    right_mat,
    prod_out,
    prod_in,
    cots_out,
    cots_in,
    cot_mat,
    cot_turned,
    grads_out,
    grads_in,
    turn_a,
    turn_b,
    wt_ref,
    gain_col,
    bias_col,
    first_ref,
    gate_ref,
    acc,
    tail,
    columns,
    from_core,
    from_plane,
    from_z,
    half,
    part,
    piece,
    all_z,
    all_plane,
    all_core,
    acc_sum,
    tail_core,
    tail_half,
    tail_plane,
    tail_part,
    tail_z,
    tail_piece,
    tail_all,
    tail_other,
    xs,
    xr,
    send_sems,
    recv_sems,
):
    core, z8, q = place()
    row = lax.axis_index("row")
    partner = device_at(1 - core, z8, q)
    barrier = pltpu.get_barrier_semaphore()
    signal(barrier, partner)
    peers(lambda dest, device: signal(barrier, device))
    looped(4, lambda i: signal(barrier, device_at(core, lax.rem(lax.div(z8, 4) * 4 + 4 + i, 8), q)))
    acc[...] = jnp.zeros_like(acc)
    tail[...] = jnp.zeros_like(tail)
    columns[...] = jnp.zeros_like(columns)
    for b in range(4):
        wt_ref[block(b)] = proj_ref[:, block(b)].T
    gain_col[...] = jnp.broadcast_to(gain_ref[1:2], (128, 128)).T
    bias_col[...] = jnp.broadcast_to(bias_ref[1:2], (128, 128)).T
    gain0, bias0 = gain_ref[0:1], bias_ref[0:1]
    gain2, bias2 = gain_ref[2:3], bias_ref[2:3]
    gate_weight = slice(512, 640)

    def enter(j):
        normed, inv = norm(place_of(pair_ref, j).astype(F32), 1)
        entered = (normed * gain0 + bias0).astype(BF16)
        return normed, inv, entered

    def keep_of(j):
        at = lax.broadcasted_iota(jnp.int32, (1, 1024), 1)
        row_at = row * 8 + lax.shift_right_logical(at, 7)
        col_at = j * 128 + jnp.bitwise_and(at, 127)
        return jnp.where(jnp.maximum(row_at, col_at) < lengths_ref[0], 1.0, 0.0)

    def start_chunk(n, j, src, dst):
        def one(dest, device):
            send(src.at[j, dest], dst.at[j, row], xs.at[n, j], xr.at[n, j], device).start()

        peers(one)
        dst[j, row] = src[j, row]

    def wait_chunk(n, j, dst):
        wait_for(dst.at[j, pl.ds(0, 63)], xr.at[n, j])

    def enter_chunk(j):
        _, _, entered = enter(j)
        keep = keep_of(j)
        pre = dot(wt_ref[...], entered, 1, 1)
        left = sigmoid(pre[0:128]) * pre[128:256] * keep
        right = sigmoid(pre[256:384]) * pre[384:512] * keep
        factors_out[j, :, 0] = to_rows(turn_a, left).astype(BF16).reshape(64, 2, 8, 128)
        factors_out[j, :, 1] = to_rows(turn_b, right).astype(BF16).reshape(64, 2, 8, 128)

        @pl.when(j == 0)
        def _():
            pl.semaphore_wait(barrier, 68)

        start_chunk(0, j, factors_out, factors_in)

    looped(CHUNKS, enter_chunk)

    def matrix(value):
        return value.astype(F32).reshape(512, 128)

    def gather_factors(j):
        wait_chunk(0, j, factors_in)
        for c in range(2):
            left_mat[c, :, column(j)] = matrix(factors_in[j, :, 0, c]).astype(BF16)
            right_mat[c, :, column(j)] = matrix(factors_in[j, :, 1, c]).astype(BF16)

    looped(CHUNKS, gather_factors)

    def product(j):
        for c in range(2):
            prod = dot(left_mat[c], right_mat[c, rows(j, 128), :], 1, 1)
            prod_out[j, :, c] = prod.reshape(64, 8, 128).astype(BF16)
        start_chunk(1, j, prod_out, prod_in)

    looped(CHUNKS, product)

    def middle(j):
        _, _, entered = enter(j)
        gate = sigmoid(dot(entered, proj_ref[:, gate_weight], 1, 0))
        cot = place_of(cot_ref, j)
        cot_t = cot.T
        wait_chunk(1, j, prod_in)
        flat = to_flat(turn_a, prod_in[j].astype(F32))
        gain1 = gain_col[:, 0:1]
        prod_normed, prod_inv = norm(flat, 0)
        prod_bf = (prod_normed * gain1 + bias_col[:, 0:1]).astype(BF16)
        update = dot(prod_bf, out_ref[...], 0, 0)
        first = (place_of(pair_ref, j).astype(F32) + gate * update).astype(BF16)
        tran_normed, tran_inv = norm(first.astype(F32), 1)
        tran_bf = (tran_normed * gain2 + bias2).astype(BF16)
        tran_t = tran_bf.T
        tran_grad = jnp.zeros((1024, 128), F32)
        for h in range(2):
            at = slice(h * 256, (h + 1) * 256)
            hidden_pre = dot(tran_bf, up_ref[:, at], 1, 0)
            hidden_sig = sigmoid(hidden_pre)
            hidden = (hidden_pre * hidden_sig).astype(BF16)
            down_term = dot(cot_t, hidden, 1, 0)
            hidden_grad = (
                dot(cot, down_ref[at, :], 1, 1)
                * hidden_sig
                * (1.0 + hidden_pre * (1.0 - hidden_sig))
            ).astype(BF16)
            up_term = dot(tran_t, hidden_grad, 1, 0)
            for k in range(2):
                acc[block(2 * h + k)] += down_term[:, block(k)]
                acc[block(4 + 2 * h + k)] += up_term[:, block(k)]
            tran_grad += dot(hidden_grad, up_ref[:, at], 1, 1)
        acc[1282:1283] += jnp.sum(tran_grad * tran_normed, axis=0, keepdims=True)
        acc[1285:1286] += jnp.sum(tran_grad, axis=0, keepdims=True)
        first_grad = norm_back(tran_grad, tran_normed, tran_inv, gain2, 1) + cot.astype(F32)
        update_grad = (first_grad * gate).astype(BF16)
        gate_grad = (first_grad * update * gate * (1.0 - gate)).astype(BF16)
        acc[block(8)] += dot(prod_bf, update_grad, 1, 0)
        norm_grad = dot(out_ref[...], update_grad, 1, 1)
        columns[:, 0:1] += jnp.sum(norm_grad * prod_normed, axis=1, keepdims=True)
        columns[:, 1:2] += jnp.sum(norm_grad, axis=1, keepdims=True)
        prod_grad = norm_back(norm_grad, prod_normed, prod_inv, gain1, 0)
        cots_out[j] = to_rows(turn_b, prod_grad).astype(BF16).reshape(64, 2, 8, 128)
        start_chunk(2, j, cots_out, cots_in)
        first_ref[:, column(j), :] = first_grad.reshape(8, 128, 128)
        gate_ref[:, column(j), :] = dot(gate_grad, proj_ref[:, gate_weight], 1, 1).reshape(8, 128, 128)
        acc[block(9)] += dot(entered.T, gate_grad, 1, 0)

    looped(CHUNKS, middle)
    for b in range(4):
        acc[block(b)] = acc[block(b)].T
    turned = columns[...].T
    acc[1281:1282] = turned[0:1]
    acc[1284:1285] = turned[1:2]

    first = send(acc.at[rows(1 - core, 1024)], from_core, send_sems.at[0], recv_sems.at[0], partner)
    first.start()
    first.wait_recv()
    half[...] = acc[rows(core, 1024)] + from_core[...]

    def to_plane(i):
        qd = lax.rem(q + i + 1, 16)
        send(half.at[rows(qd, 64)], from_plane.at[i], send_sems.at[1], recv_sems.at[1], device_at(core, z8, qd)).start()

    looped(15, to_plane)

    def gather_cots(j):
        wait_chunk(2, j, cots_in)
        for c in range(2):
            grad = matrix(cots_in[j, :, c])
            cot_mat[c, :, column(j)] = grad.astype(BF16)
            cot_turned[c, rows(j, 128), :] = grad.T.astype(BF16)

    looped(CHUNKS, gather_cots)
    wait_for(from_plane, recv_sems.at[1])
    part[...] = half[rows(q, 64)] + jnp.sum(from_plane[...], axis=0)

    def to_z(i):
        zd = lax.rem(z8 + i + 1, 8)
        send(part.at[rows(zd, 8)], from_z.at[i], send_sems.at[2], recv_sems.at[2], device_at(core, zd, q)).start()

    looped(7, to_z)

    def product_grads(j):
        for c in range(2):
            left = dot(cot_mat[c], right_mat[c, :, column(j)], 1, 0)
            right = dot(cot_turned[c], left_mat[c, :, column(j)], 1, 0)
            grads_out[j, :, 0, c] = left.reshape(64, 8, 128).astype(BF16)
            grads_out[j, :, 1, c] = right.reshape(64, 8, 128).astype(BF16)
        start_chunk(3, j, grads_out, grads_in)

    looped(CHUNKS, product_grads)
    wait_for(from_z, recv_sems.at[2])
    piece[...] = (part[rows(z8, 8)] + jnp.sum(from_z[...], axis=0)) * scale

    def back_z(i):
        send(piece, all_z.at[rows(z8, 8)], send_sems.at[3], recv_sems.at[3], device_at(core, lax.rem(z8 + i + 1, 8), q)).start()

    looped(7, back_z)
    all_z[rows(z8, 8)] = piece[...]

    def leave(j):
        normed, inv, entered = enter(j)
        keep = keep_of(j)
        pre = dot(wt_ref[...], entered, 1, 1)
        left_sig = sigmoid(pre[0:128])
        right_sig = sigmoid(pre[256:384])
        wait_chunk(3, j, grads_in)
        left = to_flat(turn_a, grads_in[j, :, 0].astype(F32)) * keep
        right = to_flat(turn_b, grads_in[j, :, 1].astype(F32)) * keep
        factor_grad = jnp.concatenate(
            [
                (left * pre[128:256] * left_sig * (1.0 - left_sig)).astype(BF16),
                (left * left_sig).astype(BF16),
                (right * pre[384:512] * right_sig * (1.0 - right_sig)).astype(BF16),
                (right * right_sig).astype(BF16),
            ],
            axis=0,
        )
        terms = dot(factor_grad, entered, 1, 0)
        for core_half in range(2):
            for b in range(16):
                at = core_half * 256 + b * 16
                to = core_half * 384 + b * 24
                tail[to : to + 16] += terms[at : at + 16]
        input_grad = dot(factor_grad, wt_ref[...], 0, 0) + place_of(gate_ref, j)
        tail[16:17] += jnp.sum(input_grad * normed, axis=0, keepdims=True)
        tail[17:18] += jnp.sum(input_grad, axis=0, keepdims=True)
        result = norm_back(input_grad, normed, inv, gain0, 1) + place_of(first_ref, j)
        grad_ref[:, column(j), :] = result.astype(BF16).reshape(8, 128, 128)

    looped(CHUNKS, leave)

    tail_first = send(tail.at[rows(1 - core, 384)], tail_core, send_sems.at[6], recv_sems.at[6], partner)
    tail_first.start()
    tail_first.wait_recv()
    tail_half[...] = tail[rows(core, 384)] + tail_core[...]

    def tail_to_plane(i):
        qd = lax.rem(q + i + 1, 16)
        send(tail_half.at[rows(qd, 24)], tail_plane.at[i], send_sems.at[7], recv_sems.at[7], device_at(core, z8, qd)).start()

    looped(15, tail_to_plane)
    wait_for(from_z, recv_sems.at[3])

    def back_plane(i):
        send(all_z, all_plane.at[rows(q, 64)], send_sems.at[4], recv_sems.at[4], device_at(core, z8, lax.rem(q + i + 1, 16))).start()

    looped(15, back_plane)
    all_plane[rows(q, 64)] = all_z[...]
    wait_for(tail_plane, recv_sems.at[7])
    tail_part[...] = (tail_half[rows(q, 24)] + jnp.sum(tail_plane[...], axis=0)) * scale

    def tail_to_z(i):
        zd = lax.rem(z8 + i + 1, 8)
        send(tail_part, tail_z.at[z8], send_sems.at[8], recv_sems.at[8], device_at(core, zd, q)).start()

    looped(7, tail_to_z)
    tail_z[z8] = tail_part[...]
    wait_for(from_plane, recv_sems.at[4])
    last = send(all_plane, all_core, send_sems.at[5], recv_sems.at[5], partner)
    last.start()
    wait_for(tail_z.at[pl.ds(0, 7)], recv_sems.at[8])
    tail_piece[...] = jnp.sum(tail_z[...], axis=0)

    def tail_back(i):
        send(tail_piece, tail_all.at[rows(q, 24)], send_sems.at[9], recv_sems.at[9], device_at(core, z8, lax.rem(q + i + 1, 16))).start()

    looped(15, tail_back)
    tail_all[rows(q, 24)] = tail_piece[...]
    last.wait_recv()
    acc_sum[rows(core, 1024)] = all_plane[...]
    acc_sum[rows(1 - core, 1024)] = all_core[...]
    for b in range(4):
        sum_down[block(b)] = acc_sum[block(b)]
        sum_up[:, block(b)] = acc_sum[block(4 + b)]
    sum_out[...] = acc_sum[block(8)]
    sum_proj[:, gate_weight] = acc_sum[block(9)]
    sum_gain[1:3] = acc_sum[1281:1283]
    sum_bias[1:3] = acc_sum[1284:1286]
    wait_for(tail_plane, recv_sems.at[9])
    tail_last = send(tail_all, tail_other, send_sems.at[10], recv_sems.at[10], partner)
    tail_last.start()

    def put_proj(which, source):
        for k in range(2):
            terms = jnp.concatenate([source[b * 24 : b * 24 + 16] for b in range(8 * k, 8 * k + 8)], axis=0)
            sum_proj[:, column(which * 2 + k)] = terms.T

    put_proj(core, tail_all)
    tail_last.wait_recv()
    put_proj(1 - core, tail_other)
    norm_terms = jnp.where(core == 0, tail_all[16:24], tail_other[16:24])
    sum_gain[0:1] = norm_terms[0:1]
    sum_bias[0:1] = norm_terms[1:2]

    first.wait_send()
    wait_for(from_plane, send_sems.at[1])
    wait_for(from_z, send_sems.at[2])
    wait_for(from_z, send_sems.at[3])
    wait_for(from_plane, send_sems.at[4])
    last.wait_send()
    tail_first.wait_send()
    wait_for(tail_plane, send_sems.at[7])
    wait_for(tail_z.at[pl.ds(0, 7)], send_sems.at[8])
    wait_for(tail_plane, send_sems.at[9])
    tail_last.wait_send()

    def settle(j):
        wait_for(factors_in.at[j, pl.ds(0, 63)], xs.at[0, j])
        wait_for(prod_in.at[j, pl.ds(0, 63)], xs.at[1, j])
        wait_for(cots_in.at[j, pl.ds(0, 63)], xs.at[2, j])
        wait_for(grads_in.at[j, pl.ds(0, 63)], xs.at[3, j])

    looped(CHUNKS, settle)


def hand_over(*refs):
    count = len(refs) // 2
    for source, target in zip(refs[:count], refs[count:]):
        target[...] = source[...]


def local(
    pair, cotangent, lengths, proj_weight, out_weight, up_weight, down_weight, norm_gain, norm_bias
):
    pair_rows = pair[0]
    cot_rows = cotangent[0]
    vmem = pl.BlockSpec(memory_space=pltpu.VMEM)
    both = (CHUNKS, 64, 2, 2, 8, 128)
    single = (CHUNKS, 64, 2, 8, 128)
    outs = pl.pallas_call(
        functools.partial(whole_kernel, 1.0 / pair_rows.shape[1]),
        out_shape=(
            jax.ShapeDtypeStruct(pair_rows.shape, BF16),
            jax.ShapeDtypeStruct(proj_weight.shape, F32),
            jax.ShapeDtypeStruct(out_weight.shape, F32),
            jax.ShapeDtypeStruct(up_weight.shape, F32),
            jax.ShapeDtypeStruct(down_weight.shape, F32),
            jax.ShapeDtypeStruct(norm_gain.shape, F32),
            jax.ShapeDtypeStruct(norm_bias.shape, F32),
        ),
        in_specs=[pl.BlockSpec(memory_space=pltpu.SMEM)] + [vmem] * 8,
        out_specs=(vmem,) * 7,
        scratch_shapes=[
            pltpu.VMEM(both, BF16),
            pltpu.VMEM(both, BF16),
            pltpu.VMEM((2, 512, 512), BF16),
            pltpu.VMEM((2, 512, 512), BF16),
            pltpu.VMEM(single, BF16),
            pltpu.VMEM(single, BF16),
            pltpu.VMEM(single, BF16),
            pltpu.VMEM(single, BF16),
            pltpu.VMEM((2, 512, 512), BF16),
            pltpu.VMEM((2, 512, 512), BF16),
            pltpu.VMEM(both, BF16),
            pltpu.VMEM(both, BF16),
            pltpu.VMEM((1024, 128), F32),
            pltpu.VMEM((1024, 128), F32),
            pltpu.VMEM((512, 128), BF16),
            pltpu.VMEM((128, 128), F32),
            pltpu.VMEM((128, 128), F32),
            pltpu.VMEM(pair_rows.shape, F32),
            pltpu.VMEM(pair_rows.shape, F32),
            pltpu.VMEM((2048, 128), F32),
            pltpu.VMEM((768, 128), F32),
            pltpu.VMEM((128, 128), F32),
            pltpu.VMEM((1024, 128), F32),
            pltpu.VMEM((15, 64, 128), F32),
            pltpu.VMEM((7, 8, 128), F32),
            pltpu.VMEM((1024, 128), F32),
            pltpu.VMEM((64, 128), F32),
            pltpu.VMEM((8, 128), F32),
            pltpu.VMEM((64, 128), F32),
            pltpu.VMEM((1024, 128), F32),
            pltpu.VMEM((1024, 128), F32),
            pltpu.VMEM((2048, 128), F32),
            pltpu.VMEM((384, 128), F32),
            pltpu.VMEM((384, 128), F32),
            pltpu.VMEM((15, 24, 128), F32),
            pltpu.VMEM((24, 128), F32),
            pltpu.VMEM((8, 24, 128), F32),
            pltpu.VMEM((24, 128), F32),
            pltpu.VMEM((384, 128), F32),
            pltpu.VMEM((384, 128), F32),
            pltpu.SemaphoreType.DMA((4, CHUNKS)),
            pltpu.SemaphoreType.DMA((4, CHUNKS)),
            pltpu.SemaphoreType.DMA((11,)),
            pltpu.SemaphoreType.DMA((11,)),
        ],
        compiler_params=pltpu.CompilerParams(
            collective_id=0, has_side_effects=True, vmem_limit_bytes=60 * 1024 * 1024
        ),
        name="whole",
    )(
        lengths,
        pair_rows,
        cot_rows,
        proj_weight,
        out_weight,
        up_weight,
        down_weight,
        norm_gain,
        norm_bias,
    )
    outs = pl.pallas_call(
        hand_over,
        out_shape=tuple(jax.ShapeDtypeStruct(o.shape, o.dtype) for o in outs),
        in_specs=[vmem] * 7,
        out_specs=(vmem,) * 7,
        name="hand_over",
    )(*outs)
    return (outs[0][None], *outs[1:])


def solution(mesh):
    in_specs = (
        P("crop", "row", None, None),
        P("crop", "row", None, None),
        P("crop"),
        P(),
        P(),
        P(),
        P(),
        P(),
        P(),
    )
    out_specs = (P("crop", "row", None, None), P(), P(), P(), P(), P(), P())
    return jax.shard_map(local, mesh=mesh, in_specs=in_specs, out_specs=out_specs, check_vma=False)
```
